128 devices in a mesh: dp: 1, cy: 16 (over z, y), cx: 8 (over x, core).
Axes of the slice: x: 4, y: 4, z: 4, core: 2. Of those that a mesh axis runs over, the one named last changes fastest.
Arguments:
- query_rows: bfloat16 [16384, 32, 128], P(('dp', 'cy', 'cx'))
- key_rows: bfloat16 [16384, 8, 128], P(('dp', 'cy', 'cx'))
- value_rows: bfloat16 [16384, 8, 128], P(('dp', 'cy', 'cx'))
- out_rows: bfloat16 [16384, 32, 128], P(('dp', 'cy', 'cx'))
- grad_out: bfloat16 [16384, 32, 128], P(('dp', 'cy', 'cx'))
- log_sum_exp: float32 [16384, 32], P(('dp', 'cy', 'cx'))
Outputs:
- output 1: bfloat16 [16384, 32, 128], P(('dp', 'cy', 'cx'))
- output 2: bfloat16 [16384, 8, 128], P(('dp', 'cy', 'cx'))
- output 3: bfloat16 [16384, 8, 128], P(('dp', 'cy', 'cx'))
All inputs are finite; a program needn't handle non-finite values.
Results may differ from the reference program's by a relative error of at most 0.0112.
Values are sent between devices in bfloat16 or wider.
A program may use at most 1 GiB of HBM per device.

```python
import math
import jax
import jax.numpy as jnp
from jax import lax

Q_HEADS = 32
KV_HEADS = 8
HEAD_DIM = 128
TOK_DEV = 128
CTX_DEVS = 128
ROW_BLOCK = 64
SEQ_LEN = CTX_DEVS * TOK_DEV
CHUNK_LEN = TOK_DEV // 2
GROUP_SIZE = Q_HEADS // KV_HEADS
N_BLOCKS = SEQ_LEN // ROW_BLOCK
SCALING = 1.0 / math.sqrt(HEAD_DIM)


def seq_positions():
    local_idx = jnp.arange(TOK_DEV, dtype=jnp.int32)
    dev_idx = jnp.arange(CTX_DEVS, dtype=jnp.int32)
    piece_id = jnp.where(local_idx[None, :] < CHUNK_LEN, dev_idx[:, None], 2 * CTX_DEVS - 1 - dev_idx[:, None])
    return (piece_id * CHUNK_LEN + local_idx[None, :] % CHUNK_LEN).reshape(SEQ_LEN)


def to_seq_order(row_data):
    split_rows = row_data.reshape((CTX_DEVS, 2, CHUNK_LEN) + row_data.shape[1:])
    return jnp.concatenate([split_rows[:, 0], split_rows[::-1, 1]], axis=0).reshape(row_data.shape)


def to_device_order(row_data):
    split_rows = row_data.reshape((2, CTX_DEVS, CHUNK_LEN) + row_data.shape[1:])
    return jnp.stack([split_rows[0], split_rows[1, ::-1]], axis=1).reshape(row_data.shape)


def forward_stats(q_seq, k_seq, v_seq):
    keys_f32 = k_seq.astype(jnp.float32)
    vals_f32 = v_seq.astype(jnp.float32)
    key_pos = jnp.arange(SEQ_LEN)
    q_blocks = q_seq.reshape(N_BLOCKS, ROW_BLOCK, KV_HEADS, GROUP_SIZE, HEAD_DIM)

    def one_block(block_in):
        q_blk, blk_idx = block_in
        query_pos = blk_idx * ROW_BLOCK + jnp.arange(ROW_BLOCK)
        keep_mask = (query_pos[:, None] >= key_pos[None, :])[None, None]
        scores = jnp.einsum('bkgd,skd->kgbs', q_blk.astype(jnp.float32), keys_f32) * SCALING
        masked = jnp.where(keep_mask, scores, -1e30)
        row_max = jnp.max(masked, axis=-1)
        exp_vals = jnp.exp(masked - row_max[..., None])
        row_sum = jnp.sum(exp_vals, axis=-1)
        prob_b16 = (exp_vals / row_sum[..., None]).astype(jnp.bfloat16)
        out_blk = jnp.einsum('kgbs,skd->bkgd', prob_b16.astype(jnp.float32), vals_f32)
        lse_blk = (row_max + jnp.log(row_sum)).transpose(2, 0, 1)
        return out_blk.astype(jnp.bfloat16).reshape(ROW_BLOCK, Q_HEADS, HEAD_DIM), lse_blk.reshape(ROW_BLOCK, Q_HEADS)

    out_blocks, lse_blocks = lax.map(one_block, (q_blocks, jnp.arange(N_BLOCKS)))
    return out_blocks.reshape(SEQ_LEN, Q_HEADS, HEAD_DIM), lse_blocks.reshape(SEQ_LEN, Q_HEADS)


def setup_inputs(seed: int = 0, part: int = 0) -> dict:
    root_key = jax.random.fold_in(jax.random.key(seed), part)
    sub_keys = jax.random.split(root_key, 6)
    shape_q = (SEQ_LEN, Q_HEADS, HEAD_DIM)
    shape_kv = (SEQ_LEN, KV_HEADS, HEAD_DIM)
    query_f32 = jax.random.normal(sub_keys[0], shape_q, jnp.float32)
    key_mean = jax.random.normal(sub_keys[1], (KV_HEADS, HEAD_DIM), jnp.float32)
    key_f32 = jax.random.normal(sub_keys[2], shape_kv, jnp.float32) + key_mean
    value_mean = jax.random.normal(sub_keys[3], (KV_HEADS, HEAD_DIM), jnp.float32)
    value_f32 = jax.random.normal(sub_keys[4], shape_kv, jnp.float32) + value_mean
    row_pos = seq_positions().astype(jnp.float32)
    dout_f32 = jax.random.normal(sub_keys[5], shape_q, jnp.float32) * jnp.sqrt((row_pos + 1.0) / 4.0)[:, None, None]
    query_rows = query_f32.astype(jnp.bfloat16)
    key_rows = key_f32.astype(jnp.bfloat16)
    value_rows = value_f32.astype(jnp.bfloat16)
    out_seq, lse_seq = forward_stats(to_seq_order(query_rows), to_seq_order(key_rows), to_seq_order(value_rows))
    return {'query_rows': query_rows, 'key_rows': key_rows, 'value_rows': value_rows, 'out_rows': to_device_order(out_seq), 'grad_out': dout_f32.astype(jnp.bfloat16), 'log_sum_exp': to_device_order(lse_seq)}


def reference(query_rows, key_rows, value_rows, out_rows, grad_out, log_sum_exp):
    q_seq = to_seq_order(query_rows)
    keys_f32 = to_seq_order(key_rows).astype(jnp.float32)
    vals_f32 = to_seq_order(value_rows).astype(jnp.float32)
    do_seq = to_seq_order(grad_out)
    delta_seq = jnp.einsum('shd,shd->sh', do_seq.astype(jnp.float32), to_seq_order(out_rows).astype(jnp.float32))
    lse_seq = to_seq_order(log_sum_exp)
    blk_shape = (N_BLOCKS, ROW_BLOCK, KV_HEADS, GROUP_SIZE)
    key_pos = jnp.arange(SEQ_LEN)

    def one_block(grad_acc, block_in):
        dk_acc, dv_acc = grad_acc
        q_blk, do_blk, lse_blk, delta_blk, blk_idx = block_in
        q_f32 = q_blk.astype(jnp.float32)
        do_f32 = do_blk.astype(jnp.float32)
        query_pos = blk_idx * ROW_BLOCK + jnp.arange(ROW_BLOCK)
        keep_mask = (query_pos[:, None] >= key_pos[None, :])[None, None]
        scores = jnp.einsum('bkgd,skd->kgbs', q_f32, keys_f32) * SCALING
        prob_f32 = jnp.where(keep_mask, jnp.exp(scores - lse_blk.transpose(1, 2, 0)[..., None]), 0.0)
        dprob_f32 = jnp.einsum('bkgd,skd->kgbs', do_f32, vals_f32)
        dscore = (prob_f32 * (dprob_f32 - delta_blk.transpose(1, 2, 0)[..., None])).astype(jnp.bfloat16).astype(jnp.float32)
        prob_rnd = prob_f32.astype(jnp.bfloat16).astype(jnp.float32)
        dq_blk = jnp.einsum('kgbs,skd->bkgd', dscore, keys_f32) * SCALING
        dk_acc = dk_acc + jnp.einsum('kgbs,bkgd->skd', dscore, q_f32)
        dv_acc = dv_acc + jnp.einsum('kgbs,bkgd->skd', prob_rnd, do_f32)
        return (dk_acc, dv_acc), dq_blk.astype(jnp.bfloat16).reshape(ROW_BLOCK, Q_HEADS, HEAD_DIM)

    zero_kv = jnp.zeros((SEQ_LEN, KV_HEADS, HEAD_DIM), jnp.float32)
    block_ins = (q_seq.reshape(blk_shape + (HEAD_DIM,)), do_seq.reshape(blk_shape + (HEAD_DIM,)), lse_seq.reshape(blk_shape), delta_seq.reshape(blk_shape), jnp.arange(N_BLOCKS))
    (dk_acc, dv_acc), dq_blocks = lax.scan(one_block, (zero_kv, zero_kv), block_ins)
    grad_query = to_device_order(dq_blocks.reshape(SEQ_LEN, Q_HEADS, HEAD_DIM))
    grad_key = to_device_order((dk_acc * SCALING).astype(jnp.bfloat16))
    grad_value = to_device_order(dv_acc.astype(jnp.bfloat16))
    return grad_query, grad_key, grad_value
```

```python
import math
import jax
import jax.numpy as jnp
from jax import lax
from jax.experimental import pallas as pl
from jax.experimental.pallas import tpu as pltpu
from jax.sharding import PartitionSpec as P

f32, bf16 = jnp.float32, jnp.bfloat16
LOG2E = 1.4426950408889634
SCALE = 1.0 / math.sqrt(128.0)
NT = (((1,), (1,)), ((), ()))
TN = (((0,), (0,)), ((), ()))
MESH = pl.DeviceIdType.MESH


def _step_j(k):
    odd = k % 2
    return odd * ((k + 1) // 2) + (1 - odd) * (8 - k // 2)


def _kernel(qd_in, st_in, kv_in, out_dq, out_dkv,
            qd, stb, st2, kv, dq, acc, rx, dqx, dqs, dks,
            loc_s, qd_s, qd_r, st_s, st_r, kvo_s, kvo_r, kvg_s, kvg_r, fw_s, fw_r,
            rs_s, rs_r, dqx_s, dqx_r, odq_s, odq_r, odk_s, odk_r):
    cy, cx = lax.axis_index("cy"), lax.axis_index("cx")
    rem, div = lax.rem, lax.div
    x, c = div(cx, 2), rem(cx, 2)
    yl, s = rem(cy, 2), div(cy, 2)
    bs = rem(s, 2)
    a = rem(yl + bs, 2)
    i = yl * 4 + x
    h = a * 4 + x

    def member(i2):
        yl2, x2 = div(i2, 4), rem(i2, 4)
        return {"cy": 2 * s + yl2, "cx": 2 * x2 + c}, rem(yl2 + bs, 2) * 4 + x2

    def peer(s2):
        return {"cy": 2 * s2 + rem(a + rem(s2, 2), 2), "cx": cx}

    partner = {"cy": cy, "cx": cx + 1 - 2 * c}

    def slot(el, i2):
        return i2 + el * (7 - 2 * i2)

    def rows(cp, el, i2):
        return pl.ds(pl.multiple_of(cp * 1024 + el * 512 + slot(el, i2) * 64, 64), 64)

    def remote(src, dst, ssem, rsem, dev):
        return pltpu.make_async_remote_copy(src, dst, ssem, rsem, device_id=dev, device_id_type=MESH)

    def arrived(ref, ssem, rsem):
        remote(ref, ref, ssem, rsem, partner).wait_recv()

    loc = [pltpu.make_async_copy(kv_in.at[h, 0], kv.at[s, 0, :, pl.ds(pl.multiple_of(i * 64, 64), 64), :], loc_s.at[0]),
           pltpu.make_async_copy(kv_in.at[h, 1], kv.at[s, 1, :, pl.ds(pl.multiple_of((7 - i) * 64, 64), 64), :], loc_s.at[1]),
           pltpu.make_async_copy(st_in.at[h], stb.at[c, i], loc_s.at[2]),
           pltpu.make_async_copy(qd_in.at[h, 1], qd.at[:, :, rows(c, 1, i), :], loc_s.at[3]),
           pltpu.make_async_copy(qd_in.at[h, 0], qd.at[:, :, rows(c, 0, i), :], loc_s.at[4])]
    for cp_ in loc:
        cp_.start()

    bar = pltpu.get_barrier_semaphore()
    pl.semaphore_signal(bar, inc=1, device_id=partner, device_id_type=MESH)
    for t in range(1, 8):
        pl.semaphore_signal(bar, inc=1, device_id=member(rem(i + t, 8))[0], device_id_type=MESH)
        pl.semaphore_signal(bar, inc=1, device_id=peer(rem(s + t, 8)), device_id_type=MESH)
    pl.semaphore_wait(bar, 15)

    sends = []

    def go(cp_):
        cp_.start()
        sends.append(cp_)

    others = [member(rem(i + t, 8)) for t in range(1, 8)]
    for t, (dev, h2) in enumerate(others):
        go(remote(kv_in.at[h2, 0], kv.at[s, 0, :, pl.ds(pl.multiple_of(i * 64, 64), 64), :], kvo_s.at[0, t], kvo_r.at[0, i], dev))
        go(remote(kv_in.at[h2, 1], kv.at[s, 1, :, pl.ds(pl.multiple_of((7 - i) * 64, 64), 64), :], kvo_s.at[1, t], kvo_r.at[1, i], dev))
        go(remote(st_in.at[h2], stb.at[c, i], st_s.at[t], st_r.at[i], dev))
    for el in (1, 0):
        for t, (dev, h2) in enumerate(others):
            go(remote(qd_in.at[h2, el], qd.at[:, :, rows(c, el, i), :], qd_s.at[el, t], qd_r.at[el, i], dev))

    def zero_acc(n, carry):
        acc[n] = jnp.zeros(acc.shape[1:], f32)
        return carry

    lax.fori_loop(0, 8, zero_acc, 0)
    for hh in range(4):
        dq[hh] = jnp.zeros(dq.shape[1:], f32)

    for el in (0, 1):
        loc[el].wait()
        for t in range(1, 8):
            i2 = rem(i + t, 8)
            arrived(kv.at[s, el, :, pl.ds(pl.multiple_of(slot(el, i2) * 64, 64), 64), :], kvo_s.at[el, t - 1], kvo_r.at[el, i2])
    for k in range(1, 8):
        s2 = rem(s + _step_j(k), 8)
        go(remote(kv.at[s, 0], kv.at[s, 0], kvg_s.at[0, k], kvg_r.at[0, s], peer(s2)))

        @pl.when(s > s2)
        def _():
            remote(kv.at[s, 1], kv.at[s, 1], kvg_s.at[1, k], kvg_r.at[1, s], peer(s2)).start()

    def build_stats(cp):
        for i2 in range(8):
            tile = jnp.transpose(stb[cp, i2])
            st2[rows(cp, 0, i2), :] = tile[:64]
            st2[rows(cp, 1, i2), :] = tile[64:]

    def half(cp, el):
        return qd.at[:, :, pl.ds(pl.multiple_of(cp * 1024 + el * 512, 512), 512), :]

    def forward(el):
        return remote(half(c, el), half(c, el), fw_s.at[el], fw_r.at[el], partner)

    loc[2].wait()
    for t in range(1, 8):
        i2 = rem(i + t, 8)
        arrived(stb.at[c, i2], st_s.at[t - 1], st_r.at[i2])
    st_fw = remote(stb.at[c], stb.at[c], fw_s.at[2], fw_r.at[2], partner)
    go(st_fw)
    build_stats(c)
    loc[3].wait()
    for t in range(1, 8):
        i2 = rem(i + t, 8)
        arrived(qd.at[:, :, rows(c, 1, i2), :], qd_s.at[1, t - 1], qd_r.at[1, i2])
    go(forward(1))

    def tiles(r0, kref, vref, dkref, dvref, pq=None, pk=None):
        def s1(hh, u):
            nk = 256 if (pq is not None and u == 0) else 512
            r = pl.ds(r0 + 256 * u, 256)
            l2 = st2[r, hh:hh + 1]
            d = st2[r, 4 + hh:5 + hh]
            sc = lax.dot_general(qd[0, hh, r, :], kref[0:nk, :], NT, preferred_element_type=f32)
            dp = lax.dot_general(qd[1, hh, r, :], vref[0:nk, :], NT, preferred_element_type=f32)
            p = jnp.exp2(sc * (SCALE * LOG2E) - l2)
            if pq is not None:
                rr = lax.broadcasted_iota(jnp.int32, (256, nk), 0) + 256 * u
                kk = lax.broadcasted_iota(jnp.int32, (256, nk), 1)
                qpos = (rr >> 6) * 128 + (rr & 63) + pq * 64
                kpos = (kk >> 6) * 128 + (kk & 63) + pk * 64
                p = jnp.where(qpos >= kpos, p, 0.0)
            return p.astype(bf16), (p * (dp - d)).astype(bf16)

        todo = [(hh, u) for u in range(2) for hh in range(4)]
        now = s1(*todo[0])
        for n, (hh, u) in enumerate(todo):
            nxt = s1(*todo[n + 1]) if n + 1 < len(todo) else None
            pb, ds = now
            nk = pb.shape[1]
            r = pl.ds(r0 + 256 * u, 256)
            dkref[:, 0:nk] += lax.dot_general(qd[0, hh, r, :], ds, TN, preferred_element_type=f32)
            dvref[:, 0:nk] += lax.dot_general(qd[1, hh, r, :], pb, TN, preferred_element_type=f32)
            dq[hh, r, :] += jnp.dot(ds, kref[0:nk, :], preferred_element_type=f32)
            now = nxt

    def send_acc(k, g, kel):
        remote(acc.at[k, kel], rx.at[s, kel], rs_s.at[kel, k], rs_r.at[kel, s], peer(g)).start()

    def full_unit(n, carry):
        k, u = div(n + 2, 4), rem(n + 2, 4)
        live = div(k + 7, 8)
        sub = div(u, 2) * live
        g = rem(s + 8 - _step_j(k) * live, 8)
        gt = div(g - s + 7, 8)
        el = 1 - sub + sub * gt
        kel = sub * gt
        cp = rem(c + u, 2)

        @pl.when(n == 1)
        def _():
            arrived(stb.at[1 - c], fw_s.at[2], fw_r.at[2])
            build_stats(1 - c)
            arrived(half(1 - c, 1), fw_s.at[1], fw_r.at[1])

        @pl.when(n == 2)
        def _():
            loc[4].wait()
            for t in range(1, 8):
                i2 = rem(i + t, 8)
                arrived(qd.at[:, :, rows(c, 0, i2), :], qd_s.at[0, t - 1], qd_r.at[0, i2])
            forward(0).start()

        @pl.when(n == 4)
        def _():
            arrived(half(1 - c, 0), fw_s.at[0], fw_r.at[0])

        @pl.when((n >= 2) & (u == 0))
        def _():
            arrived(kv.at[g, 0], kvg_s.at[0, k], kvg_r.at[0, g])

        @pl.when((n >= 2) & (u == 2) & (gt == 1))
        def _():
            arrived(kv.at[g, 1], kvg_s.at[1, k], kvg_r.at[1, g])

        r0 = pl.multiple_of(cp * 1024 + el * 512, 512)
        tiles(r0, kv.at[g, kel, 0], kv.at[g, kel, 1], acc.at[k, kel, 0], acc.at[k, kel, 1])

        @pl.when((n >= 2) & (((u == 1) & (gt == 1)) | ((u == 3) & (gt == 0))))
        def _():
            send_acc(k, g, 0)

        @pl.when((n >= 2) & (u == 3) & (gt == 1))
        def _():
            send_acc(k, g, 1)

        return carry

    lax.fori_loop(0, 30, full_unit, 0)

    def dqx_copy(el):
        src = dq.at[:, pl.ds(pl.multiple_of((1 - c) * 1024 + el * 512, 512), 512), :]
        return remote(src, dqx.at[el], dqx_s.at[el], dqx_r.at[el], partner)

    def finish_dq(el):
        arrived(dqx.at[el], dqx_s.at[el], dqx_r.at[el])
        mine = pl.ds(pl.multiple_of(c * 1024 + el * 512, 512), 512)
        for hh in range(4):
            dqs[el, hh] = ((dq[hh, mine, :] + dqx[el, hh]) * SCALE).astype(bf16)

        def block(i2):
            return dqs.at[el, :, pl.ds(pl.multiple_of(slot(el, i2) * 64, 64), 64), :]

        for t in range(1, 8):
            i2 = rem(i + t, 8)
            remote(block(i2), out_dq.at[h, el], odq_s.at[el, t], odq_r.at[el, h], member(i2)[0]).start()
        pltpu.make_async_copy(block(i), out_dq.at[h, el], odq_s.at[el, 0]).start()

    def diag_unit(m, carry):
        el = div(m, 2)
        cp = rem(c + 1 + m, 2)
        r0 = pl.multiple_of(cp * 1024 + el * 512, 512)
        tiles(r0, kv.at[s, el, 0], kv.at[s, el, 1], acc.at[0, el, 0], acc.at[0, el, 1],
              pq=rem(cp + el, 2), pk=rem(c + el, 2))

        @pl.when(rem(m, 2) == 0)
        def _():
            dqx_copy(el).start()

        @pl.when(rem(m, 2) == 1)
        def _():
            finish_dq(el)

        return carry

    lax.fori_loop(0, 4, diag_unit, 0)

    for el in (0, 1):
        for k in range(1, 8):
            s3 = rem(s + _step_j(k), 8)

            def take():
                arrived(rx.at[s3, el], rs_s.at[el, k], rs_r.at[el, s3])
                acc[0, el] += rx[s3, el]

            if el == 0:
                take()
            else:
                pl.when(s > s3)(take)
        dks[el, 0] = (jnp.transpose(acc[0, el, 0]) * SCALE).astype(bf16)
        dks[el, 1] = jnp.transpose(acc[0, el, 1]).astype(bf16)

        def kblock(i2):
            return dks.at[el, :, pl.ds(pl.multiple_of(slot(el, i2) * 64, 64), 64), :]

        for t in range(1, 8):
            i2 = rem(i + t, 8)
            remote(kblock(i2), out_dkv.at[h, el], odk_s.at[el, t], odk_r.at[el, h], member(i2)[0]).start()
        pltpu.make_async_copy(kblock(i), out_dkv.at[h, el], odk_s.at[el, 0]).start()

    for cp_ in sends:
        cp_.wait_send()
    forward(0).wait_send()
    for k in range(1, 8):
        s2 = rem(s + _step_j(k), 8)

        @pl.when(s > s2)
        def _():
            remote(kv.at[s, 1], kv.at[s, 1], kvg_s.at[1, k], kvg_r.at[1, s], peer(s2)).wait_send()

        g = rem(s + 8 - _step_j(k), 8)
        remote(acc.at[k, 0], rx.at[s, 0], rs_s.at[0, k], rs_r.at[0, s], peer(g)).wait_send()

        @pl.when(g > s)
        def _():
            remote(acc.at[k, 1], rx.at[s, 1], rs_s.at[1, k], rs_r.at[1, s], peer(g)).wait_send()
    for el in (0, 1):
        dqx_copy(el).wait_send()
        pltpu.make_async_copy(dqs.at[el, :, pl.ds(0, 64), :], out_dq.at[h, el], odq_s.at[el, 0]).wait()
        pltpu.make_async_copy(dks.at[el, :, pl.ds(0, 64), :], out_dkv.at[h, el], odk_s.at[el, 0]).wait()
        for t in range(1, 8):
            dev, h2 = member(rem(i + t, 8))
            remote(dqs.at[el, :, pl.ds(0, 64), :], out_dq.at[h, el], odq_s.at[el, t], odq_r.at[el, h], dev).wait_send()
            remote(dks.at[el, :, pl.ds(0, 64), :], out_dkv.at[h, el], odk_s.at[el, t], odk_r.at[el, h], dev).wait_send()
            arrived(out_dq.at[h2, el], odq_s.at[el, t], odq_r.at[el, h2])
            arrived(out_dkv.at[h2, el], odk_s.at[el, t], odk_r.at[el, h2])


def solution(mesh):
    row_spec = P(('dp', 'cy', 'cx'), None, None)
    stat_spec = P(('dp', 'cy', 'cx'), None)

    def local(q, k, v, o, do, lse):
        T, H, D = q.shape
        G = k.shape[1]
        R = H // G
        half = T // 2
        delta = jnp.sum(do.astype(f32) * o.astype(f32), axis=-1)
        st_in = jnp.stack([lse * LOG2E, delta]).reshape(2, T, G, R).transpose(2, 0, 3, 1).reshape(G, 2 * R, T)
        qd_in = jnp.stack([q, do]).reshape(2, 2, half, G, R, D).transpose(3, 1, 0, 4, 2, 5)
        kv_in = jnp.stack([k, v]).reshape(2, 2, half, G, D).transpose(3, 1, 0, 2, 4)
        hbm = pl.BlockSpec(memory_space=pl.ANY)
        V, S = pltpu.VMEM, pltpu.SemaphoreType.DMA
        dq_o, dkv_o = pl.pallas_call(
            _kernel,
            in_specs=[hbm] * 3,
            out_specs=[hbm] * 2,
            out_shape=[jax.ShapeDtypeStruct((G, 2, R, half, D), bf16), jax.ShapeDtypeStruct((G, 2, 2, half, D), bf16)],
            scratch_shapes=[
                V((2, R, 2048, D), bf16), V((2, 8, 8, T), f32), V((2048, 8), f32), V((8, 2, 2, 512, D), bf16),
                V((R, 2048, D), f32), V((8, 2, 2, D, 512), f32), V((8, 2, 2, D, 512), f32), V((2, R, 512, D), f32),
                V((2, R, 512, D), bf16), V((2, 2, 512, D), bf16),
                S((5,)), S((2, 7)), S((2, 8)), S((7,)), S((8,)), S((2, 7)), S((2, 8)), S((2, 8)), S((2, 8)), S((3,)), S((3,)),
                S((2, 8)), S((2, 8)), S((2,)), S((2,)), S((2, 8)), S((2, 8)), S((2, 8)), S((2, 8)),
            ],
            compiler_params=pltpu.CompilerParams(collective_id=0, has_side_effects=True, vmem_limit_bytes=60 << 20),
            cost_estimate=pl.CostEstimate(flops=46 << 30, bytes_accessed=8 << 20, transcendentals=36 << 20),
            name="attn_bwd",
        )(qd_in, st_in, kv_in)
        grad_q = dq_o.transpose(1, 3, 0, 2, 4).reshape(T, H, D)
        grad_kv = dkv_o.transpose(2, 1, 3, 0, 4).reshape(2, T, G, D)
        return grad_q, grad_kv[0], grad_kv[1]

    return jax.shard_map(local, mesh=mesh, in_specs=(row_spec,) * 5 + (stat_spec,), out_specs=(row_spec,) * 3, check_vma=False)
```

```python
import math
import jax
import jax.numpy as jnp
from jax import lax
from jax.experimental import pallas as pl
from jax.experimental.pallas import tpu as pltpu
from jax.sharding import PartitionSpec as P

f32, bf16 = jnp.float32, jnp.bfloat16
LOG2E = 1.4426950408889634
SCALE = 1.0 / math.sqrt(128.0)
NT = (((1,), (1,)), ((), ()))
TN = (((0,), (0,)), ((), ()))
MESH = pl.DeviceIdType.MESH
BOTH, NEAR, AROUND = (0, 1), (1, 3), (1, 3, 2)
STEPS = (("c1", "s3", "s1", "c3", "c2", "c0", "s2"), ("c1", "c3", "s1", "c2", "s3", "c0", "s2"))
PASS = ("00s3E9", "00s3L3+", "00s1E4", "00s1L5+", "00s2E12", "00s2L13",
        "12s1E4", "33s1E5", "11s1L5+", "22s1L6", "13s3E9", "11s2E12", "11s2L13", "23s2E13")

def _pick(k, values):
    r = values[0]
    for n in range(1, len(values)):
        r = jnp.where(k == n, values[n], r)
    return r


def _kernel(q_in, do_in, l_in, d_in, k_in, v_in, out_dq, out_dk, out_dv,
            qd, stb, st2, kv, dq, acc, rxy, rxz, rzf, dqx, dqs, dks,
            in_s, ql_r, fl_s, fl_r, kvg_s, kvg_r, ry_s, ry_r, rz_s, rz_r, odk_s, odk_r, dqx_s, dqx_r,
            kvo_r, st_r, qe_r, fe_s, fe_r, zf_s, zf_r, odq_s, odq_r):
    cy, cx = lax.axis_index("cy"), lax.axis_index("cx")
    rem, div = lax.rem, lax.div
    x, c = div(cx, 2), rem(cx, 2)
    yl, s = rem(cy, 2), div(cy, 2)
    z, bs = div(s, 2), rem(s, 2)
    a = rem(yl + bs, 2)
    i = yl * 4 + x
    h = a * 4 + x
    pair = 2 * z + 1 - bs

    def member(i2):
        yl2, x2 = div(i2, 4), rem(i2, 4)
        return {"cy": 2 * s + yl2, "cx": 2 * x2 + c}, rem(yl2 + bs, 2) * 4 + x2

    def peer(s2):
        return {"cy": 2 * s2 + rem(a + rem(s2, 2), 2), "cx": cx}

    across = peer(pair)
    partner = {"cy": cy, "cx": cx + 1 - 2 * c}
    others = [member(rem(i + t, 8)) for t in range(1, 8)]

    def block(el, i2):
        return pl.ds(pl.multiple_of((i2 + el * (7 - 2 * i2)) * 64, 64), 64)

    def half(cp, el):
        return pl.ds(pl.multiple_of(cp * 1024 + el * 512, 512), 512)

    def rows(cp, el, i2):
        return pl.ds(pl.multiple_of(cp * 1024 + el * 512 + (i2 + el * (7 - 2 * i2)) * 64, 64), 64)

    def remote(src, dst, ssem, rsem, dev):
        return pltpu.make_async_remote_copy(src, dst, ssem, rsem, device_id=dev, device_id_type=MESH)

    def arrived(ref, rsem):
        remote(ref, ref, in_s.at[0], rsem, partner).wait_recv()

    def sent(ref, ssem):
        remote(ref, ref, ssem, st_r.at[0], partner).wait_send()

    for el in BOTH:
        for n, src in enumerate((k_in, v_in)):
            pltpu.make_async_copy(src.at[h, el], kv.at[s, el, n, block(el, i), :], kvo_r.at[el]).start()
    for n, src in enumerate((l_in, d_in)):
        pltpu.make_async_copy(src.at[h], stb.at[c, i, n], st_r.at[0]).start()
    for n, src in enumerate((q_in, do_in)):
        for hh in range(4):
            pltpu.make_async_copy(src.at[h, 1, hh], qd.at[n, hh, rows(c, 1, i), :], ql_r.at[hh]).start()
        pltpu.make_async_copy(src.at[h, 0], qd.at[n, :, rows(c, 0, i), :], qe_r.at[0]).start()

    bar = pltpu.get_barrier_semaphore()
    pl.semaphore_signal(bar, inc=1, device_id=partner, device_id_type=MESH)
    pl.semaphore_signal(bar, inc=1, device_id=across, device_id_type=MESH)
    for dev, _ in others:
        pl.semaphore_signal(bar, inc=1, device_id=dev, device_id_type=MESH)
    for d in range(1, 4):
        pl.semaphore_signal(bar, inc=1, device_id=peer(2 * rem(z + d, 4) + bs), device_id_type=MESH)
    pl.semaphore_wait(bar, 12)

    for el in BOTH:
        for dev, h2 in others:
            for n, src in enumerate((k_in, v_in)):
                remote(src.at[h2, el], kv.at[s, el, n, block(el, i), :], in_s.at[n], kvo_r.at[el], dev).start()
    for dev, h2 in others:
        for n, src in enumerate((l_in, d_in)):
            remote(src.at[h2], stb.at[c, i, n], in_s.at[4 + n], st_r.at[0], dev).start()
    for hh in range(4):
        for dev, h2 in others:
            for n, src in enumerate((q_in, do_in)):
                remote(src.at[h2, 1, hh], qd.at[n, hh, rows(c, 1, i), :], in_s.at[2 + n], ql_r.at[hh], dev).start()
    for dev, h2 in others:
        for n, src in enumerate((q_in, do_in)):
            remote(src.at[h2, 0], qd.at[n, :, rows(c, 0, i), :], in_s.at[2 + n], qe_r.at[0], dev).start()

    def zero_acc(n, carry):
        acc[n] = jnp.zeros(acc.shape[1:], f32)
        return carry

    lax.fori_loop(0, 8, zero_acc, 0)
    for hh in range(4):
        dq[hh] = jnp.zeros(dq.shape[1:], f32)

    def spread(g, el, d, n):
        return remote(kv.at[g, el], kv.at[g, el], kvg_s.at[el, n], kvg_r.at[el, g], peer(2 * rem(z + 4 - d, 4) + bs))

    def spread_all(g, el, n0, ds, act):
        for d in ds:
            if el == 0:
                act(spread(g, el, d, n0 + d))
            else:
                pl.when(z > rem(z + 4 - d, 4))(lambda: act(spread(g, el, d, n0 + d)))

    def to_across(el):
        return remote(kv.at[s, el], kv.at[s, el], kvg_s.at[el, 0], kvg_r.at[el, s], across)

    def start(cp):
        cp.start()

    for el in BOTH:
        arrived(kv.at[s, el], kvo_r.at[el])
        to_across(el).start()
        spread_all(s, el, 0, NEAR, start)

    def build_stats(cp):
        for i2 in range(8):
            for n, factor in enumerate((LOG2E, 1.0)):
                tile = jnp.transpose(stb[cp, i2, n] * factor)
                for el in BOTH:
                    st2[rows(cp, el, i2), 4 * n:4 * n + 4] = tile[64 * el:64 * el + 64]

    st_fw = remote(stb.at[c], stb.at[c], fe_s.at[1], fe_r.at[1], partner)
    arrived(stb.at[c], st_r.at[0])
    st_fw.start()
    build_stats(c)

    def fw_late(hh):
        return remote(qd.at[:, hh, half(c, 1), :], qd.at[:, hh, half(c, 1), :], fl_s.at[hh], fl_r.at[hh], partner)

    def fw_early():
        return remote(qd.at[:, :, half(c, 0), :], qd.at[:, :, half(c, 0), :], fe_s.at[0], fe_r.at[0], partner)

    def scores(hh, r, kref, vref, nk, l2, d, mask=None):
        sc = lax.dot_general(qd[0, hh, r, :], kref[0:nk, :], NT, preferred_element_type=f32)
        dp = lax.dot_general(qd[1, hh, r, :], vref[0:nk, :], NT, preferred_element_type=f32)
        p = jnp.exp2(sc * (SCALE * LOG2E) - l2)
        if mask is not None:
            u, pq, pk = mask
            rr = lax.broadcasted_iota(jnp.int32, (256, nk), 0) + 256 * u
            kk = lax.broadcasted_iota(jnp.int32, (256, nk), 1)
            qpos = (rr >> 6) * 128 + (rr & 63) + pq * 64
            kpos = (kk >> 6) * 128 + (kk & 63) + pk * 64
            p = jnp.where(qpos >= kpos, p, 0.0)
        return p.astype(bf16), (p * (dp - d)).astype(bf16)

    def terms(hh, r, kref, dkref, dvref, nk, pb, ds):
        dkref[:, 0:nk] += lax.dot_general(qd[0, hh, r, :], ds, TN, preferred_element_type=f32)
        dvref[:, 0:nk] += lax.dot_general(qd[1, hh, r, :], pb, TN, preferred_element_type=f32)
        dq[hh, r, :] += jnp.dot(ds, kref[0:nk, :], preferred_element_type=f32)

    def pipelined(todo):
        now = todo[0][0]()
        for n in range(len(todo)):
            nxt = todo[n + 1][0]() if n + 1 < len(todo) else None
            todo[n][1](*now)
            now = nxt

    def tiles(bases, kref, vref, dkref, dvref, masks=None):
        def pair_of(n, hh, u):
            nk = 512 if masks is None or u == 1 else 256
            r = pl.ds(bases[n] + 256 * u, 256)
            mask = None if masks is None else (u, *masks[n])
            return (lambda: scores(hh, r, kref, vref, nk, st2[r, hh:hh + 1], st2[r, 4 + hh:5 + hh], mask),
                    lambda pb, ds: terms(hh, r, kref, dkref, dvref, nk, pb, ds))
        pipelined([pair_of(n, hh, u) for n in range(len(bases)) for u in range(2) for hh in range(4)])

    def heads_in(hh):
        arrived(qd.at[:, hh, half(c, 1), :], ql_r.at[hh])
        fw_late(hh).start()

    def partner_heads_in(hh):
        arrived(qd.at[:, hh, half(1 - c, 1), :], fl_r.at[hh])

    def own_tiles(hh, cp):
        r0 = pl.multiple_of(cp * 1024 + 512, 512)

        def pair_of(el, u):
            nk = 256 if el > u else 512
            r = pl.ds(r0 + 256 * u, 256)
            mask = None if el == 0 else (u, rem(cp + 1, 2), rem(c + 1, 2))
            kref, vref = kv.at[s, el, 0], kv.at[s, el, 1]

            def first():
                st = pltpu.roll(st2[r, :], rem(128 - hh, 128), 1)
                return scores(hh, r, kref, vref, nk, st[:, 0:1], st[:, 4:5], mask)

            return first, lambda pb, ds: terms(hh, r, kref, acc.at[0, el, 0], acc.at[0, el, 1], nk, pb, ds)

        pipelined([pair_of(el, u) for el in range(2) for u in range(2)])

    def own_unit(m, carry):
        hh, other = div(m, 2), rem(m, 2)

        @pl.when(other == 0)
        def _():
            heads_in(hh)

        @pl.when(m == 1)
        def _():
            arrived(stb.at[1 - c], fe_r.at[1])
            build_stats(1 - c)
            arrived(kv.at[pair, 0], kvg_r.at[0, pair])
            spread_all(pair, 0, 3, NEAR, start)

        @pl.when(m == 3)
        def _():
            arrived(kv.at[pair, 1], kvg_r.at[1, pair])
            spread_all(pair, 1, 3, NEAR, start)
            for el in BOTH:
                spread_all(s, el, 0, (2,), start)
                spread_all(pair, el, 3, (2,), start)

        @pl.when(other == 1)
        def _():
            partner_heads_in(hh)

        own_tiles(hh, rem(c + m, 2))
        return carry

    def late_heads(cp):
        lax.fori_loop(2, 4, lambda hh, carry: own_tiles(hh, cp), None)

    lax.fori_loop(0, 4, own_unit, 0)
    for hh in (2, 3):
        heads_in(hh)
    late_heads(c)
    for hh in (2, 3):
        partner_heads_in(hh)

    def acc_y(k, d, kel):
        return remote(acc.at[k + 1, kel], rxy.at[d, kel], ry_s.at[kel, d], ry_r.at[kel, d], across)

    def acc_z(k, d, kel):
        return remote(acc.at[k + 1, kel], rxz.at[z, kel], rz_s.at[kel, d], rz_r.at[kel, z], peer(2 * rem(z + d, 4) + bs))

    def acc_f(k, d):
        return remote(acc.at[k + 1, 1], rzf, zf_s.at[rem(d, 2) * div(d, 2)], zf_r.at[0], peer(2 * rem(z + d, 4) + bs))

    def by_z_first(d):
        return ((z == 0) & (rem(d, 2) == 1)) | ((z == 1) & (d == 1))

    def step_of(k):
        d, cross = (jnp.where(z == 0, *(_pick(k, [of(name) for name in order]) for order in STEPS))
                    for of in (lambda name: int(name[1]), lambda name: int(name[0] == "c")))
        g = 2 * rem(z + d, 4) + rem(bs + cross, 2)
        return d, cross, g, div(g - s + 7, 8)

    def pass_at(n):
        for entry in PASS:
            z_lo, z_hi, d, kel = int(entry[0]), int(entry[1]), int(entry[3]), "EL".index(entry[4])
            k = STEPS[min(z_lo, 1)].index(entry[2:4])

            def go_on():
                if not entry.endswith("+"):
                    arrived(rxy.at[d, kel], ry_r.at[kel, d])
                    acc[k + 1, kel] += rxy[d, kel]
                acc_z(k, d, kel).start()

            pl.when((n == int(entry[5:].rstrip("+"))) & (z >= z_lo) & (z <= z_hi))(go_on)

    def late_across(k, d):
        zfirst = by_z_first(d)

        @pl.when(zfirst)
        def _():
            acc_f(k, d).start()

        @pl.when((d == 0) & (z > 0))
        def _():
            arrived(rzf, zf_r.at[0])
            acc[k + 1, 1] += rzf[...]

        @pl.when(jnp.logical_not(zfirst))
        def _():
            acc_y(k, d, 1).start()

    def full_unit(n, carry):
        k, sub = div(n, 2), rem(n, 2)
        d, cross, g, gt = step_of(k)
        el = 1 - sub + sub * gt
        kel = sub * gt

        last = div(z, 3)

        @pl.when(n == 2 - last)
        def _():
            pl.when(z == 3)(lambda: late_heads(1 - c))
            arrived(qd.at[:, :, half(c, 0), :], qe_r.at[0])
            fw_early().start()

        @pl.when(n == 3 - 2 * last)
        def _():
            arrived(qd.at[:, :, half(1 - c, 0), :], fe_r.at[0])

        @pl.when((sub == 0) & (d > 0))
        def _():
            arrived(kv.at[g, 0], kvg_r.at[0, g])

        @pl.when((sub == 1) & (d > 0) & (gt == 1))
        def _():
            arrived(kv.at[g, 1], kvg_r.at[1, g])

        bases = [pl.multiple_of(cp * 1024 + el * 512, 512) for cp in (c, 1 - c)]
        tiles(bases, kv.at[g, kel, 0], kv.at[g, kel, 1], acc.at[k + 1, kel, 0], acc.at[k + 1, kel, 1])

        @pl.when((cross == 1) & (sub == gt) & ((gt == 1) | ((d == 0) & (z > 0))))
        def _():
            late_across(k, d)

        @pl.when((cross == 1) & (sub == 1 - gt))
        def _():
            acc_y(k, d, 0).start()

        pass_at(n)
        return carry

    lax.fori_loop(0, 14, full_unit, 0)

    def heads(p):
        return pl.ds(2 * p, 2)

    def dqx_copy(el, p):
        return remote(dq.at[heads(p), half(1 - c, el), :], dqx.at[el, heads(p)], dqx_s.at[el, p], dqx_r.at[el, p], partner)

    def finish_dq(el, p):
        arrived(dqx.at[el, heads(p)], dqx_r.at[el, p])
        for hh in (2 * p, 2 * p + 1):
            dqs[el, hh] = ((dq[hh, half(c, el), :] + dqx[el, hh]) * SCALE).astype(bf16)
        out = out_dq.at[h, heads(p), el]
        for t, (dev, _) in enumerate(others):
            remote(dqs.at[el, heads(p), block(el, rem(i + t + 1, 8)), :], out, odq_s.at[el], odq_r.at[el], dev).start()
        pltpu.make_async_copy(dqs.at[el, heads(p), block(el, i), :], out, odq_r.at[el]).start()

    dqx_copy(1, 0).start()

    def diag_unit(m, carry):
        cp = rem(c + 1 + m, 2)
        kd, vd = kv.at[s, 0, 0], kv.at[s, 0, 1]
        tiles([pl.multiple_of(cp * 1024, 512)], kd, vd, acc.at[0, 0, 0], acc.at[0, 0, 1], [(cp, c)])

        @pl.when(m == 0)
        def _():
            for p in BOTH:
                dqx_copy(0, p).start()
            finish_dq(1, 0)

        return carry

    lax.fori_loop(0, 2, diag_unit, 0)
    for p in BOTH:
        finish_dq(0, p)
    pl.when(z < 3)(lambda: late_heads(1 - c))
    dqx_copy(1, 1).start()
    finish_dq(1, 1)

    def take(ref, rsem, el):
        arrived(ref, rsem)
        acc[0, el] += ref[...]

    for el in BOTH:
        for d in AROUND:
            zs = rem(z + d, 4)

            def take_z():
                take(rxz.at[zs, el], rz_r.at[el, zs], el)

            take_z() if el == 0 else pl.when(z > zs)(take_z)

        def take_y():
            take(rxy.at[0, el], ry_r.at[el, 0], el)

        take_y() if el == 0 else pl.when((bs == 1) | (z > 0))(take_y)
        dks[el, 0] = (jnp.transpose(acc[0, el, 0]) * SCALE).astype(bf16)
        dks[el, 1] = jnp.transpose(acc[0, el, 1]).astype(bf16)
        for n, out in enumerate((out_dk, out_dv)):
            for t, (dev, _) in enumerate(others):
                remote(dks.at[el, n, block(el, rem(i + t + 1, 8)), :], out.at[h, el], odk_s.at[el, n], odk_r.at[el, n], dev).start()
            pltpu.make_async_copy(dks.at[el, n, block(el, i), :], out.at[h, el], odk_r.at[el, n]).start()

    for n, src in enumerate((k_in, v_in, q_in, do_in, l_in, d_in)):
        sent(src.at[pl.ds(0, 7)], in_s.at[n])
    for el in BOTH:
        to_across(el).wait_send()
        spread_all(s, el, 0, AROUND, lambda cp: cp.wait_send())
        spread_all(pair, el, 3, AROUND, lambda cp: cp.wait_send())
    st_fw.wait_send()
    fw_early().wait_send()
    for hh in range(4):
        fw_late(hh).wait_send()
    for k, name in enumerate(STEPS[0]):
        d, cross = int(name[1]), int(name[0] == "c")
        made = acc_y if cross else acc_z
        made(k, d, 0).wait_send()
        later = 2 * rem(z + d, 4) + rem(bs + cross, 2) > s
        if not cross:
            pl.when(later)(lambda: made(k, d, 1).wait_send())
        elif d == 0:
            pl.when(later | (z > 0))(lambda: made(k, d, 1).wait_send())
        else:
            zfirst = by_z_first(d)
            pl.when(zfirst)(lambda: acc_f(k, d).wait_send())
            pl.when(later & jnp.logical_not(zfirst))(lambda: made(k, d, 1).wait_send())
    for el in BOTH:
        for p in BOTH:
            dqx_copy(el, p).wait_send()
        sent(dqs.at[el, :, pl.ds(0, 448), :], odq_s.at[el])
        arrived(out_dq.at[:, :, el], odq_r.at[el])
        for n, out in enumerate((out_dk, out_dv)):
            sent(dks.at[el, n, pl.ds(0, 448), :], odk_s.at[el, n])
            arrived(out.at[:, el], odk_r.at[el, n])


def solution(mesh):
    row_spec = P(('dp', 'cy', 'cx'), None, None)
    stat_spec = P(('dp', 'cy', 'cx'), None)

    def local(q, k, v, o, do, lse):
        T, H, D = q.shape
        G = k.shape[1]
        R = H // G
        half = T // 2
        delta = jnp.sum(do.astype(f32) * o.astype(f32), axis=-1)
        l_in, d_in = (t.T.reshape(G, R, T) for t in (lse, delta))
        q_in, do_in = (t.reshape(2, half, G, R, D).transpose(2, 0, 3, 1, 4) for t in (q, do))
        k_in, v_in = (t.reshape(2, half, G, D).transpose(2, 0, 1, 3) for t in (k, v))
        hbm = pl.BlockSpec(memory_space=pl.ANY)
        V, S = pltpu.VMEM, pltpu.SemaphoreType.DMA
        S2, W = 2 * G * T, G * half
        dq_o, dk_o, dv_o = pl.pallas_call(
            _kernel,
            in_specs=[hbm] * 6,
            out_specs=[hbm] * 3,
            out_shape=[jax.ShapeDtypeStruct((G, R, 2, half, D), bf16)] + [jax.ShapeDtypeStruct((G, 2, half, D), bf16)] * 2,
            scratch_shapes=[
                V((2, R, S2, D), bf16), V((2, G, 2, R, T), f32), V((S2, T), f32), V((G, 2, 2, W, D), bf16), V((R, S2, D), f32),
                V((G, 2, 2, D, W), f32), V((4, 2, 2, D, W), f32), V((4, 2, 2, D, W), f32), V((2, D, W), f32), V((2, R, W, D), f32),
                V((2, R, W, D), bf16), V((2, 2, W, D), bf16),
                *[S((G,))] * 4, *[S((2, G))] * 10, *[S((2,))] * 9,
            ],
            compiler_params=pltpu.CompilerParams(collective_id=0, has_side_effects=True, vmem_limit_bytes=60 << 20),
            cost_estimate=pl.CostEstimate(flops=46 << 30, bytes_accessed=8 << 20, transcendentals=36 << 20),
            name="attn_bwd",
        )(q_in, do_in, l_in, d_in, k_in, v_in)
        grad_q = dq_o.reshape(H, T, D).transpose(1, 0, 2)
        grad_k, grad_v = (t.reshape(G, T, D).transpose(1, 0, 2) for t in (dk_o, dv_o))
        return grad_q, grad_k, grad_v

    return jax.shard_map(local, mesh=mesh, in_specs=(row_spec,) * 5 + (stat_spec,), out_specs=(row_spec,) * 3, check_vma=False)
```

```python
import math
import jax
import jax.numpy as jnp
from jax import lax
from jax.experimental import pallas as pl
from jax.experimental.pallas import tpu as pltpu
from jax.sharding import PartitionSpec as P

f32, bf16 = jnp.float32, jnp.bfloat16
LOG2E = 1.4426950408889634
SCALE = 1.0 / math.sqrt(128.0)
NT = (((1,), (1,)), ((), ()))
TN = (((0,), (0,)), ((), ()))
MESH = pl.DeviceIdType.MESH
BOTH, NEAR, AROUND = (0, 1), (1, 3), (1, 3, 2)
STEPS = (("c1", "s1", "s3", "c3", "c2", "c0", "s2"), ("c1", "c3", "s1", "c2", "s3", "c0", "s2"), ("c1", "c3", "s1", "c2", "s2", "c0", "s3"))
PASS = ("00s3E9", "00s3L5+", "00s1E4", "00s1L3+", "00s2E12", "00s2L14",
        "12s1E4", "33s1E5", "11s1L5+", "22s1L6", "11s3E9", "11s2E12", "11s2L13", "23s2E10", "23s3E13")

def _pick(k, values):
    r = values[0]
    for n in range(1, len(values)):
        r = jnp.where(k == n, values[n], r)
    return r


def _kernel(q, do, o, k, v, l_in, out_dq, out_dk, out_dv,
            qn, don, on, kn, vn, wide_q, wide_o, q_in, do_in, k_in, v_in, d_in, dqr, dkr, dvr,
            qd, stb, st2, kv, dq, acc, rxy, rxz, rzf, dqx, dqs, dks, nat_s,
            in_s, ql_r, fl_s, fl_r, kvg_s, kvg_r, ry_s, ry_r, rz_s, rz_r, odk_s, odk_r, dqx_s, dqx_r,
            loc_s, kvo_r, st_r, qe_r, fe_s, fe_r, zf_s, zf_r, odq_s, odq_r):
    cy, cx = lax.axis_index("cy"), lax.axis_index("cx")
    T = q.shape[0]
    rem, div = lax.rem, lax.div
    x, c = div(cx, 2), rem(cx, 2)
    yl, s = rem(cy, 2), div(cy, 2)
    z, bs = div(s, 2), rem(s, 2)
    a = rem(yl + bs, 2)
    i = yl * 4 + x
    h = a * 4 + x
    pair = 2 * z + 1 - bs

    def member(i2):
        yl2, x2 = div(i2, 4), rem(i2, 4)
        return {"cy": 2 * s + yl2, "cx": 2 * x2 + c}, rem(yl2 + bs, 2) * 4 + x2

    def peer(s2):
        return {"cy": 2 * s2 + rem(a + rem(s2, 2), 2), "cx": cx}

    across = peer(pair)
    partner = {"cy": cy, "cx": cx + 1 - 2 * c}
    others = [member(rem(i + t, 8)) for t in range(1, 8)]
    seven = pl.ds(0, 7 * 64)

    def block(el, i2):
        return pl.ds(pl.multiple_of((i2 + el * (7 - 2 * i2)) * 64, 64), 64)

    def half(cp, el):
        return pl.ds(pl.multiple_of(cp * 1024 + el * 512, 512), 512)

    def rows(cp, el, i2):
        return pl.ds(pl.multiple_of(cp * 1024 + el * 512 + (i2 + el * (7 - 2 * i2)) * 64, 64), 64)

    def remote(src, dst, ssem, rsem, dev):
        return pltpu.make_async_remote_copy(src, dst, ssem, rsem, device_id=dev, device_id_type=MESH)

    def arrived(ref, rsem):
        remote(ref, ref, in_s.at[0], rsem, partner).wait_recv()

    def sent(ref, ssem):
        remote(ref, ref, ssem, st_r.at[0], partner).wait_send()

    natives = [pltpu.make_async_copy(src, dst, nat_s.at[n]) for n, (src, dst) in enumerate(((k, kn), (v, vn), (q, qn), (do, don), (o, on)))]
    for cp_ in natives:
        cp_.start()
    pltpu.make_async_copy(l_in.at[h], stb.at[c, i, 0], loc_s.at[0]).start()

    bar = pltpu.get_barrier_semaphore()
    pl.semaphore_signal(bar, inc=1, device_id=partner, device_id_type=MESH)
    pl.semaphore_signal(bar, inc=1, device_id=across, device_id_type=MESH)
    for dev, _ in others:
        pl.semaphore_signal(bar, inc=1, device_id=dev, device_id_type=MESH)
    for d in range(1, 4):
        pl.semaphore_signal(bar, inc=1, device_id=peer(2 * rem(z + d, 4) + bs), device_id_type=MESH)

    def widen(ref, wide):
        heads_ = ref.shape[1]
        for t in range(0, ref.shape[0], 16):
            wide[pl.ds(t * heads_, 16 * heads_), :] = ref[pl.ds(t, 16)].astype(f32).reshape(16 * heads_, ref.shape[2])

    def of_head(wide, j, heads_):
        return wide[pl.ds(j, T, stride=heads_), :]

    for n, (ref, dst) in enumerate(((kn, k_in), (vn, v_in))):
        natives[n].wait()
        widen(ref, wide_o)
        for j in range(8):
            rows_ = of_head(wide_o, j, 8).astype(bf16)
            for el in BOTH:
                dst[j, el] = rows_[64 * el:64 * el + 64]
        for el in BOTH:
            kv[s, el, n, block(el, i), :] = dst[h, el]
    def by_head(n, ref, dst, stats):
        natives[2 + n].wait()
        widen(ref, wide_q)
        if stats:
            natives[4].wait()
            widen(on, wide_o)
        for j in range(32):
            rows_ = of_head(wide_q, j, 32)
            for el in BOTH:
                dst[j // 4, el, j % 4] = rows_[64 * el:64 * el + 64].astype(bf16)
            if stats:
                terms_ = rows_ * of_head(wide_o, j, 32)
                d_in[j // 4, pl.ds(j % 4, 1), :] = jnp.sum(jnp.transpose(terms_), axis=0, keepdims=True)
        for el in BOTH:
            qd[n, :, rows(c, el, i), :] = dst[h, el]

    by_head(0, qn, q_in, False)
    def zero_acc(n, carry):
        acc[n] = jnp.zeros(acc.shape[1:], f32)
        return carry

    lax.fori_loop(0, 8, zero_acc, 0)
    for hh in range(4):
        dq[hh] = jnp.zeros(dq.shape[1:], f32)

    pl.semaphore_wait(bar, 12)
    for el in BOTH:
        for dev, h2 in others:
            for n, src in enumerate((k_in, v_in)):
                remote(src.at[h2, el], kv.at[s, el, n, block(el, i), :], in_s.at[n], kvo_r.at[el], dev).start()
    by_head(1, don, do_in, True)
    stb[c, i, 1] = d_in[h]

    def spread(g, el, d, n):
        return remote(kv.at[g, el], kv.at[g, el], kvg_s.at[el, n], kvg_r.at[el, g], peer(2 * rem(z + 4 - d, 4) + bs))

    def spread_all(g, el, n0, ds, act):
        for d in ds:
            if el == 0:
                act(spread(g, el, d, n0 + d))
            else:
                pl.when(z > rem(z + 4 - d, 4))(lambda: act(spread(g, el, d, n0 + d)))

    def to_across(el):
        return remote(kv.at[s, el], kv.at[s, el], kvg_s.at[el, 0], kvg_r.at[el, s], across)

    def start(cp):
        cp.start()

    def send_stats():
        for dev, h2 in others:
            for n, src in enumerate((l_in, d_in)):
                remote(src.at[h2], stb.at[c, i, n], in_s.at[4 + n], st_r.at[0], dev).start()

    def send_late():
        for hh in range(4):
            for dev, h2 in others:
                for n, src in enumerate((q_in, do_in)):
                    remote(src.at[h2, 1, hh], qd.at[n, hh, rows(c, 1, i), :], in_s.at[2 + n], ql_r.at[hh], dev).start()

    def send_early():
        for dev, h2 in others:
            for n, src in enumerate((q_in, do_in)):
                remote(src.at[h2, 0], qd.at[n, :, rows(c, 0, i), :], in_s.at[2 + n], qe_r.at[0], dev).start()

    for el in BOTH:
        arrived(kv.at[s, el, :, seven], kvo_r.at[el])
        to_across(el).start()
        spread_all(s, el, 0, NEAR if el == 0 else (3,), start)
        if el == 0:
            send_stats()
            send_late()

    def build_stats(cp):
        for i2 in range(8):
            for n, factor in enumerate((LOG2E, 1.0)):
                tile = jnp.transpose(stb[cp, i2, n] * factor)
                for el in BOTH:
                    st2[rows(cp, el, i2), 4 * n:4 * n + 4] = tile[64 * el:64 * el + 64]

    st_fw = remote(stb.at[c], stb.at[c], fe_s.at[1], fe_r.at[1], partner)
    arrived(stb.at[c, pl.ds(0, 7)], st_r.at[0])
    pltpu.make_async_copy(l_in.at[h], stb.at[c, i, 0], loc_s.at[0]).wait()
    st_fw.start()
    build_stats(c)

    def fw_late(hh):
        return remote(qd.at[:, hh, half(c, 1), :], qd.at[:, hh, half(c, 1), :], fl_s.at[hh], fl_r.at[hh], partner)

    def fw_early():
        return remote(qd.at[:, :, half(c, 0), :], qd.at[:, :, half(c, 0), :], fe_s.at[0], fe_r.at[0], partner)

    def scores(hh, r, kref, vref, nk, l2, d, mask=None):
        sc = lax.dot_general(qd[0, hh, r, :], kref[0:nk, :], NT, preferred_element_type=f32)
        dp = lax.dot_general(qd[1, hh, r, :], vref[0:nk, :], NT, preferred_element_type=f32)
        p = jnp.exp2(sc * (SCALE * LOG2E) - l2)
        if mask is not None:
            u, pq, pk = mask
            rr = lax.broadcasted_iota(jnp.int32, (256, nk), 0) + 256 * u
            kk = lax.broadcasted_iota(jnp.int32, (256, nk), 1)
            qpos = (rr >> 6) * 128 + (rr & 63) + pq * 64
            kpos = (kk >> 6) * 128 + (kk & 63) + pk * 64
            p = jnp.where(qpos >= kpos, p, 0.0)
        return p.astype(bf16), (p * (dp - d)).astype(bf16)

    def terms(hh, r, kref, dkref, dvref, nk, pb, ds):
        dkref[:, 0:nk] += lax.dot_general(qd[0, hh, r, :], ds, TN, preferred_element_type=f32)
        dvref[:, 0:nk] += lax.dot_general(qd[1, hh, r, :], pb, TN, preferred_element_type=f32)
        dq[hh, r, :] += jnp.dot(ds, kref[0:nk, :], preferred_element_type=f32)

    def pipelined(todo):
        now = todo[0][0]()
        for n in range(len(todo)):
            nxt = todo[n + 1][0]() if n + 1 < len(todo) else None
            todo[n][1](*now)
            now = nxt

    def tiles(bases, kref, vref, dkref, dvref, masks=None):
        def pair_of(n, hh, u):
            nk = 512 if masks is None or u == 1 else 256
            r = pl.ds(bases[n] + 256 * u, 256)
            mask = None if masks is None else (u, *masks[n])
            return (lambda: scores(hh, r, kref, vref, nk, st2[r, hh:hh + 1], st2[r, 4 + hh:5 + hh], mask),
                    lambda pb, ds: terms(hh, r, kref, dkref, dvref, nk, pb, ds))
        pipelined([pair_of(n, hh, u) for n in range(len(bases)) for u in range(2) for hh in range(4)])

    def heads_in(hh):
        arrived(qd.at[:, hh, seven], ql_r.at[hh])
        fw_late(hh).start()

    def partner_heads_in(hh):
        arrived(qd.at[:, hh, half(1 - c, 1), :], fl_r.at[hh])

    def own_tiles(hh, cp):
        r0 = pl.multiple_of(cp * 1024 + 512, 512)

        def pair_of(el, u):
            nk = 256 if el > u else 512
            r = pl.ds(r0 + 256 * u, 256)
            mask = None if el == 0 else (u, rem(cp + 1, 2), rem(c + 1, 2))
            kref, vref = kv.at[s, el, 0], kv.at[s, el, 1]

            def first():
                st = pltpu.roll(st2[r, :], rem(128 - hh, 128), 1)
                return scores(hh, r, kref, vref, nk, st[:, 0:1], st[:, 4:5], mask)

            return first, lambda pb, ds: terms(hh, r, kref, acc.at[0, el, 0], acc.at[0, el, 1], nk, pb, ds)

        pipelined([pair_of(el, u) for el in range(2) for u in range(2)])

    def own_unit(m, carry):
        hh, other = div(m, 2), rem(m, 2)

        @pl.when(other == 0)
        def _():
            heads_in(hh)

        @pl.when(m == 1)
        def _():
            arrived(stb.at[1 - c], fe_r.at[1])
            build_stats(1 - c)
            arrived(kv.at[pair, 0], kvg_r.at[0, pair])
            spread_all(pair, 0, 3, NEAR, start)

        @pl.when(m == 3)
        def _():
            arrived(kv.at[pair, 1], kvg_r.at[1, pair])
            spread_all(pair, 1, 3, NEAR, start)
            spread_all(s, 1, 0, (1,), start)
            for el in BOTH:
                spread_all(s, el, 0, (2,), start)
                spread_all(pair, el, 3, (2,), start)

        @pl.when(other == 1)
        def _():
            partner_heads_in(hh)

        own_tiles(hh, rem(c + m, 2))
        return carry

    def late_heads(cp):
        lax.fori_loop(2, 4, lambda hh, carry: own_tiles(hh, cp), None)

    send_early()
    lax.fori_loop(0, 4, own_unit, 0)
    for hh in (2, 3):
        heads_in(hh)
    late_heads(c)
    for hh in (2, 3):
        partner_heads_in(hh)

    def acc_y(k, d, kel):
        return remote(acc.at[k + 1, kel], rxy.at[d, kel], ry_s.at[kel, d], ry_r.at[kel, d], across)

    def acc_z(k, d, kel):
        return remote(acc.at[k + 1, kel], rxz.at[z, kel], rz_s.at[kel, d], rz_r.at[kel, z], peer(2 * rem(z + d, 4) + bs))

    def acc_f(k, d):
        return remote(acc.at[k + 1, 1], rzf, zf_s.at[rem(d, 2) * div(d, 2)], zf_r.at[0], peer(2 * rem(z + d, 4) + bs))

    def by_z_first(d):
        return ((z == 0) & (rem(d, 2) == 1)) | ((z == 1) & (d == 1))

    def step_of(k):
        d, cross = (_pick(z, [_pick(k, [of(name) for name in order]) for order in (*STEPS, STEPS[2])])
                    for of in (lambda name: int(name[1]), lambda name: int(name[0] == "c")))
        g = 2 * rem(z + d, 4) + rem(bs + cross, 2)
        return d, cross, g, div(g - s + 7, 8)

    def pass_at(n):
        for entry in PASS:
            z_lo, z_hi, d, kel = int(entry[0]), int(entry[1]), int(entry[3]), "EL".index(entry[4])
            k = STEPS[min(z_lo, 2)].index(entry[2:4])

            def go_on():
                if not entry.endswith("+"):
                    arrived(rxy.at[d, kel], ry_r.at[kel, d])
                    acc[k + 1, kel] += rxy[d, kel]
                acc_z(k, d, kel).start()

            pl.when((n == int(entry[5:].rstrip("+"))) & (z >= z_lo) & (z <= z_hi))(go_on)

    def late_across(k, d):
        zfirst = by_z_first(d)

        @pl.when(zfirst)
        def _():
            acc_f(k, d).start()

        @pl.when((d == 0) & (z > 0))
        def _():
            arrived(rzf, zf_r.at[0])
            acc[k + 1, 1] += rzf[...]

        @pl.when(jnp.logical_not(zfirst))
        def _():
            acc_y(k, d, 1).start()

    def heads(p):
        return pl.ds(2 * p, 2)

    def dqx_copy(el, p):
        return remote(dq.at[heads(p), half(1 - c, el), :], dqx.at[el, heads(p)], dqx_s.at[el, p], dqx_r.at[el, p], partner)

    def finish_dq(el, p):
        arrived(dqx.at[el, heads(p)], dqx_r.at[el, p])
        for hh in (2 * p, 2 * p + 1):
            dqs[el, hh] = ((dq[hh, half(c, el), :] + dqx[el, hh]) * SCALE).astype(bf16)
        for t, (dev, _) in enumerate(others):
            remote(dqs.at[el, heads(p), block(el, rem(i + t + 1, 8)), :], dqr.at[h, heads(p), el], odq_s.at[el], odq_r.at[el], dev).start()
        dqr[h, heads(p), el] = dqs[el, heads(p), block(el, i), :]

    def full_unit(n, carry):
        k, sub = div(n, 2), rem(n, 2)
        d, cross, g, gt = step_of(k)
        el = 1 - sub + sub * gt
        kel = sub * gt

        last = div(z, 3)

        @pl.when(n == 2 - last)
        def _():
            pl.when(z == 3)(lambda: late_heads(1 - c))
            arrived(qd.at[:, :, seven], qe_r.at[0])
            fw_early().start()

        @pl.when(n == 3 - 2 * last)
        def _():
            arrived(qd.at[:, :, half(1 - c, 0), :], fe_r.at[0])

        @pl.when((sub == 0) & (d > 0))
        def _():
            arrived(kv.at[g, 0], kvg_r.at[0, g])

        @pl.when((sub == 1) & (d > 0) & (gt == 1))
        def _():
            arrived(kv.at[g, 1], kvg_r.at[1, g])

        bases = [pl.multiple_of(cp * 1024 + el * 512, 512) for cp in (c, 1 - c)]
        tiles(bases, kv.at[g, kel, 0], kv.at[g, kel, 1], acc.at[k + 1, kel, 0], acc.at[k + 1, kel, 1])

        @pl.when((cross == 1) & (sub == gt) & ((gt == 1) | ((d == 0) & (z > 0))))
        def _():
            late_across(k, d)

        @pl.when((cross == 1) & (sub == 1 - gt))
        def _():
            acc_y(k, d, 0).start()

        pass_at(n)

        @pl.when(n == 13 - div(z, 2))
        def _():
            dqx_copy(1, 0).start()
            pl.when(z == 3)(lambda: dqx_copy(1, 1).start())

        return carry

    lax.fori_loop(0, 14, full_unit, 0)

    @pl.when(z >= 2)
    def _():
        finish_dq(1, 0)
        pl.when(z == 3)(lambda: finish_dq(1, 1))

    def diag_unit(m, carry):
        cp = rem(c + 1 + m, 2)
        kd, vd = kv.at[s, 0, 0], kv.at[s, 0, 1]
        tiles([pl.multiple_of(cp * 1024, 512)], kd, vd, acc.at[0, 0, 0], acc.at[0, 0, 1], [(cp, c)])

        @pl.when(m == 0)
        def _():
            for p in BOTH:
                dqx_copy(0, p).start()
            pass_at(14)
            pl.when(z < 2)(lambda: finish_dq(1, 0))

        return carry

    lax.fori_loop(0, 2, diag_unit, 0)
    for p in BOTH:
        finish_dq(0, p)

    @pl.when(z < 3)
    def _():
        late_heads(1 - c)
        dqx_copy(1, 1).start()
        finish_dq(1, 1)


    def take(ref, rsem, el):
        arrived(ref, rsem)
        acc[0, el] += ref[...]

    for el in BOTH:
        for d in AROUND:
            zs = rem(z + d, 4)

            def take_z():
                take(rxz.at[zs, el], rz_r.at[el, zs], el)

            take_z() if el == 0 else pl.when(z > zs)(take_z)

        def take_y():
            take(rxy.at[0, el], ry_r.at[el, 0], el)

        take_y() if el == 0 else pl.when((bs == 1) | (z > 0))(take_y)
        dks[el, 0] = (jnp.transpose(acc[0, el, 0]) * SCALE).astype(bf16)
        dks[el, 1] = jnp.transpose(acc[0, el, 1]).astype(bf16)
        for n, got in enumerate((dkr, dvr)):
            for t, (dev, _) in enumerate(others):
                remote(dks.at[el, n, block(el, rem(i + t + 1, 8)), :], got.at[h, el], odk_s.at[el, n], odk_r.at[el, n], dev).start()
            got[h, el] = dks[el, n, block(el, i), :]

    def by_token(got, el, heads_, wide, out):
        for j in range(heads_):
            wide[pl.ds(j + 64 * el * heads_, 64, stride=heads_), :] = got(j).astype(f32)
        for t in range(64 * el, 64 * el + 64, 16):
            out[pl.ds(t, 16)] = wide[pl.ds(t * heads_, 16 * heads_), :].reshape(16, heads_, out.shape[2]).astype(bf16)

    for el in BOTH:
        arrived(dqr.at[pl.ds(0, 7), :, el], odq_r.at[el])
        by_token(lambda j: dqr[j // 4, j % 4, el], el, 32, wide_q, out_dq)
    for el in BOTH:
        for n, (got, out) in enumerate(((dkr, out_dk), (dvr, out_dv))):
            arrived(got.at[pl.ds(0, 7), el], odk_r.at[el, n])
            by_token(lambda j: got[j, el], el, 8, wide_o, out)

    for n, src in enumerate((k_in, v_in, q_in, do_in, l_in, d_in)):
        sent(src.at[pl.ds(0, 7)], in_s.at[n])
    for el in BOTH:
        to_across(el).wait_send()
        spread_all(s, el, 0, AROUND, lambda cp: cp.wait_send())
        spread_all(pair, el, 3, AROUND, lambda cp: cp.wait_send())
    st_fw.wait_send()
    fw_early().wait_send()
    for hh in range(4):
        fw_late(hh).wait_send()
    for k, name in enumerate(STEPS[0]):
        d, cross = int(name[1]), int(name[0] == "c")
        made = acc_y if cross else acc_z
        made(k, d, 0).wait_send()
        later = 2 * rem(z + d, 4) + rem(bs + cross, 2) > s
        if not cross:
            pl.when(later)(lambda: made(k, d, 1).wait_send())
        elif d == 0:
            pl.when(later | (z > 0))(lambda: made(k, d, 1).wait_send())
        else:
            zfirst = by_z_first(d)
            pl.when(zfirst)(lambda: acc_f(k, d).wait_send())
            pl.when(later & jnp.logical_not(zfirst))(lambda: made(k, d, 1).wait_send())
    for el in BOTH:
        for p in BOTH:
            dqx_copy(el, p).wait_send()
        sent(dqs.at[el, :, pl.ds(0, 448), :], odq_s.at[el])
        for n in BOTH:
            sent(dks.at[el, n, pl.ds(0, 448), :], odk_s.at[el, n])


def solution(mesh):
    row_spec = P(('dp', 'cy', 'cx'), None, None)
    stat_spec = P(('dp', 'cy', 'cx'), None)

    def local(q, k, v, o, do, lse):
        T, H, D = q.shape
        G = k.shape[1]
        R = H // G
        half = T // 2
        l_in = lse.T.reshape(G, R, T)
        hbm = pl.BlockSpec(memory_space=pl.ANY)
        V, S = pltpu.VMEM, pltpu.SemaphoreType.DMA
        S2, W = 2 * G * T, G * half
        return pl.pallas_call(
            _kernel,
            in_specs=[hbm] * 6,
            out_specs=[pl.BlockSpec(memory_space=pltpu.VMEM)] * 3,
            out_shape=[V((T, H, D), bf16)] + [V((T, G, D), bf16)] * 2,
            scratch_shapes=[
                *[V((T, H, D), bf16)] * 3, *[V((T, G, D), bf16)] * 2, *[V((T * H, D), f32)] * 2,
                *[V((G, 2, R, half, D), bf16)] * 2, *[V((G, 2, half, D), bf16)] * 2, V((G, R, T), f32),
                V((G, R, 2, half, D), bf16), *[V((G, 2, half, D), bf16)] * 2,
                V((2, R, S2, D), bf16), V((2, G, 2, R, T), f32), V((S2, T), f32), V((G, 2, 2, W, D), bf16), V((R, S2, D), f32),
                V((G, 2, 2, D, W), f32), V((4, 2, 2, D, W), f32), V((4, 2, 2, D, W), f32), V((2, D, W), f32), V((2, R, W, D), f32),
                V((2, R, W, D), bf16), V((2, 2, W, D), bf16),
                *[S((G,))] * 5, *[S((2, G))] * 10, *[S((2,))] * 10,
            ],
            compiler_params=pltpu.CompilerParams(collective_id=0, has_side_effects=True, vmem_limit_bytes=60 << 20),
            cost_estimate=pl.CostEstimate(flops=46 << 30, bytes_accessed=8 << 20, transcendentals=36 << 20),
            name="attn_bwd",
        )(q, do, o, k, v, l_in)

    return jax.shard_map(local, mesh=mesh, in_specs=(row_spec,) * 5 + (stat_spec,), out_specs=(row_spec,) * 3, check_vma=False)
```

```python
import math
import jax
import jax.numpy as jnp
from jax import lax
from jax.experimental import pallas as pl
from jax.experimental.pallas import tpu as pltpu
from jax.sharding import PartitionSpec as P

f32, bf16 = jnp.float32, jnp.bfloat16
LOG2E = 1.4426950408889634
SCALE = 1.0 / math.sqrt(128.0)
NT = (((1,), (1,)), ((), ()))
TN = (((0,), (0,)), ((), ()))
MESH = pl.DeviceIdType.MESH
BOTH, NEAR, AROUND = (0, 1), (1, 3), (1, 3, 2)
STEPS = (("c1", "s1", "s3", "c3", "c2", "c0", "s2"), ("c1", "c3", "s1", "c2", "s3", "c0", "s2"), ("c1", "c3", "s1", "c2", "s2", "c0", "s3"))
PASS = ("00s3E9", "00s3L5+", "00s1E4", "00s1L3+", "00s2E12", "00s2L14v",
        "12s1E4", "33s1E5", "11s1L5+", "22s1L6", "11s3E9", "11s2E12", "11s2L13", "23s2E10", "23s3E13")

def _pick(k, values):
    r = values[0]
    for n in range(1, len(values)):
        r = jnp.where(k == n, values[n], r)
    return r


def _kernel(q, do, o, k, v, l_in, out_dq, out_dk, out_dv,
            qn, don, on, kn, vn, wide_q, wide_o, q_in, do_in, k_in, v_in, d_in, dqr, dkr, dvr,
            qd, stb, st2, kv, dq, acc, rxy, rxz, rzf, dqx, dqs, dks,
            nat_s, in_s, ql_r, fl_s, fl_r, zf_s, zf_r, kvg_s, kvg_r, ry_s, ry_r, rz_s, rz_r, odk_s, odk_r, dqx_s, dqx_r,
            loc_s, kvo_r, st_r, qe_r, fe_s, fe_r, odq_s, odq_r):
    cy, cx = lax.axis_index("cy"), lax.axis_index("cx")
    T = q.shape[0]
    rem, div = lax.rem, lax.div
    x, c = div(cx, 2), rem(cx, 2)
    yl, s = rem(cy, 2), div(cy, 2)
    z, bs = div(s, 2), rem(s, 2)
    a = rem(yl + bs, 2)
    i = yl * 4 + x
    h = a * 4 + x
    pair = 2 * z + 1 - bs

    def member(i2):
        yl2, x2 = div(i2, 4), rem(i2, 4)
        return {"cy": 2 * s + yl2, "cx": 2 * x2 + c}, rem(yl2 + bs, 2) * 4 + x2

    def peer(s2):
        return {"cy": 2 * s2 + rem(a + rem(s2, 2), 2), "cx": cx}

    across = peer(pair)
    partner = {"cy": cy, "cx": cx + 1 - 2 * c}
    others = [member(rem(i + t, 8)) for t in range(1, 8)]
    seven = pl.ds(0, 7 * 64)

    def block(el, i2):
        return pl.ds(pl.multiple_of((i2 + el * (7 - 2 * i2)) * 64, 64), 64)

    def half(cp, el):
        return pl.ds(pl.multiple_of(cp * 1024 + el * 512, 512), 512)

    def rows(cp, el, i2):
        return pl.ds(pl.multiple_of(cp * 1024 + el * 512 + (i2 + el * (7 - 2 * i2)) * 64, 64), 64)

    def remote(src, dst, ssem, rsem, dev):
        return pltpu.make_async_remote_copy(src, dst, ssem, rsem, device_id=dev, device_id_type=MESH)

    def arrived(ref, rsem):
        remote(ref, ref, in_s.at[0], rsem, partner).wait_recv()

    def sent(ref, ssem):
        remote(ref, ref, ssem, st_r.at[0], partner).wait_send()

    natives = [pltpu.make_async_copy(src, dst, nat_s.at[n]) for n, (src, dst) in enumerate(((k, kn), (v, vn), (q, qn), (do, don), (o, on)))]
    for cp_ in natives:
        cp_.start()
    pltpu.make_async_copy(l_in.at[h], stb.at[c, i, 0], loc_s.at[0]).start()

    bar = pltpu.get_barrier_semaphore()
    pl.semaphore_signal(bar, inc=1, device_id=partner, device_id_type=MESH)
    pl.semaphore_signal(bar, inc=1, device_id=across, device_id_type=MESH)
    for dev, _ in others:
        pl.semaphore_signal(bar, inc=1, device_id=dev, device_id_type=MESH)
    for d in range(1, 4):
        pl.semaphore_signal(bar, inc=1, device_id=peer(2 * rem(z + d, 4) + bs), device_id_type=MESH)

    def widen(ref, wide):
        heads_ = ref.shape[1]
        for t in range(0, ref.shape[0], 16):
            wide[pl.ds(t * heads_, 16 * heads_), :] = ref[pl.ds(t, 16)].astype(f32).reshape(16 * heads_, ref.shape[2])

    def of_head(wide, j, heads_):
        return wide[pl.ds(j, T, stride=heads_), :]

    for n, (ref, dst) in enumerate(((kn, k_in), (vn, v_in))):
        natives[n].wait()
        widen(ref, wide_o)
        for j in range(8):
            rows_ = of_head(wide_o, j, 8).astype(bf16)
            for el in BOTH:
                dst[j, el] = rows_[64 * el:64 * el + 64]
        for el in BOTH:
            kv[s, el, n, block(el, i), :] = dst[h, el]
    def by_head(n, ref, dst, stats):
        natives[2 + n].wait()
        widen(ref, wide_q)
        if stats:
            natives[4].wait()
            widen(on, wide_o)
        for j in range(32):
            rows_ = of_head(wide_q, j, 32)
            for el in BOTH:
                dst[j // 4, el, j % 4] = rows_[64 * el:64 * el + 64].astype(bf16)
            if stats:
                terms_ = rows_ * of_head(wide_o, j, 32)
                d_in[j // 4, pl.ds(j % 4, 1), :] = jnp.sum(jnp.transpose(terms_), axis=0, keepdims=True)
        for el in BOTH:
            qd[n, :, rows(c, el, i), :] = dst[h, el]

    by_head(0, qn, q_in, False)
    def zero_acc(n, carry):
        acc[n] = jnp.zeros(acc.shape[1:], f32)
        return carry

    lax.fori_loop(0, 8, zero_acc, 0)
    for hh in range(4):
        dq[hh] = jnp.zeros(dq.shape[1:], f32)

    pl.semaphore_wait(bar, 12)
    for el in BOTH:
        for dev, h2 in others:
            for n, src in enumerate((k_in, v_in)):
                remote(src.at[h2, el], kv.at[s, el, n, block(el, i), :], in_s.at[n], kvo_r.at[el], dev).start()
    by_head(1, don, do_in, True)
    stb[c, i, 1] = d_in[h]

    def spread(g, el, d, n):
        return remote(kv.at[g, el], kv.at[g, el], kvg_s.at[el, n], kvg_r.at[el, g], peer(2 * rem(z + 4 - d, 4) + bs))

    def spread_all(g, el, n0, ds, act):
        for d in ds:
            if el == 0:
                act(spread(g, el, d, n0 + d))
            else:
                pl.when(z > rem(z + 4 - d, 4))(lambda: act(spread(g, el, d, n0 + d)))

    def to_across(el):
        return remote(kv.at[s, el], kv.at[s, el], kvg_s.at[el, 0], kvg_r.at[el, s], across)

    def start(cp):
        cp.start()

    def send_stats():
        for dev, h2 in others:
            for n, src in enumerate((l_in, d_in)):
                remote(src.at[h2], stb.at[c, i, n], in_s.at[4 + n], st_r.at[0], dev).start()

    def send_late():
        for hh in range(4):
            for dev, h2 in others:
                for n, src in enumerate((q_in, do_in)):
                    remote(src.at[h2, 1, hh], qd.at[n, hh, rows(c, 1, i), :], in_s.at[2 + n], ql_r.at[hh], dev).start()

    def send_early():
        for dev, h2 in others:
            for n, src in enumerate((q_in, do_in)):
                remote(src.at[h2, 0], qd.at[n, :, rows(c, 0, i), :], in_s.at[2 + n], qe_r.at[0], dev).start()

    for el in BOTH:
        arrived(kv.at[s, el, :, seven], kvo_r.at[el])
        to_across(el).start()
        spread_all(s, el, 0, NEAR if el == 0 else (3,), start)
        if el == 0:
            send_stats()
            send_late()

    def build_stats(cp):
        for i2 in range(8):
            for n, factor in enumerate((LOG2E, 1.0)):
                tile = jnp.transpose(stb[cp, i2, n] * factor)
                for el in BOTH:
                    st2[rows(cp, el, i2), 4 * n:4 * n + 4] = tile[64 * el:64 * el + 64]

    st_fw = remote(stb.at[c], stb.at[c], fe_s.at[1], fe_r.at[1], partner)
    arrived(stb.at[c, pl.ds(0, 7)], st_r.at[0])
    pltpu.make_async_copy(l_in.at[h], stb.at[c, i, 0], loc_s.at[0]).wait()
    st_fw.start()
    build_stats(c)

    def fw_late(hh):
        return remote(qd.at[:, hh, half(c, 1), :], qd.at[:, hh, half(c, 1), :], fl_s.at[hh], fl_r.at[hh], partner)

    def fw_early():
        return remote(qd.at[:, :, half(c, 0), :], qd.at[:, :, half(c, 0), :], fe_s.at[0], fe_r.at[0], partner)

    def scores(hh, r, kref, vref, nk, l2, d, mask=None):
        sc = lax.dot_general(qd[0, hh, r, :], kref[0:nk, :], NT, preferred_element_type=f32)
        dp = lax.dot_general(qd[1, hh, r, :], vref[0:nk, :], NT, preferred_element_type=f32)
        p = jnp.exp2(sc * (SCALE * LOG2E) - l2)
        if mask is not None:
            u, pq, pk = mask
            rr = lax.broadcasted_iota(jnp.int32, (256, nk), 0) + 256 * u
            kk = lax.broadcasted_iota(jnp.int32, (256, nk), 1)
            qpos = (rr >> 6) * 128 + (rr & 63) + pq * 64
            kpos = (kk >> 6) * 128 + (kk & 63) + pk * 64
            p = jnp.where(qpos >= kpos, p, 0.0)
        return p.astype(bf16), (p * (dp - d)).astype(bf16)

    def terms(hh, r, kref, dkref, dvref, nk, pb, ds):
        dkref[:, 0:nk] += lax.dot_general(qd[0, hh, r, :], ds, TN, preferred_element_type=f32)
        dvref[:, 0:nk] += lax.dot_general(qd[1, hh, r, :], pb, TN, preferred_element_type=f32)
        dq[hh, r, :] += jnp.dot(ds, kref[0:nk, :], preferred_element_type=f32)

    def pipelined(todo):
        now = todo[0][0]()
        for n in range(len(todo)):
            nxt = todo[n + 1][0]() if n + 1 < len(todo) else None
            todo[n][1](*now)
            now = nxt

    def tiles(bases, kref, vref, dkref, dvref, masks=None):
        def pair_of(n, hh, u):
            nk = 512 if masks is None or u == 1 else 256
            r = pl.ds(bases[n] + 256 * u, 256)
            mask = None if masks is None else (u, *masks[n])
            return (lambda: scores(hh, r, kref, vref, nk, st2[r, hh:hh + 1], st2[r, 4 + hh:5 + hh], mask),
                    lambda pb, ds: terms(hh, r, kref, dkref, dvref, nk, pb, ds))
        pipelined([pair_of(n, hh, u) for n in range(len(bases)) for u in range(2) for hh in range(4)])

    def heads_in(hh):
        arrived(qd.at[:, hh, seven], ql_r.at[hh])
        fw_late(hh).start()

    def partner_heads_in(hh):
        arrived(qd.at[:, hh, half(1 - c, 1), :], fl_r.at[hh])

    def own_tiles(hh, cp):
        r0 = pl.multiple_of(cp * 1024 + 512, 512)

        def pair_of(el, u):
            nk = 256 if el > u else 512
            r = pl.ds(r0 + 256 * u, 256)
            mask = None if el == 0 else (u, rem(cp + 1, 2), rem(c + 1, 2))
            kref, vref = kv.at[s, el, 0], kv.at[s, el, 1]

            def first():
                st = pltpu.roll(st2[r, :], rem(128 - hh, 128), 1)
                return scores(hh, r, kref, vref, nk, st[:, 0:1], st[:, 4:5], mask)

            return first, lambda pb, ds: terms(hh, r, kref, acc.at[0, el, 0], acc.at[0, el, 1], nk, pb, ds)

        pipelined([pair_of(el, u) for el in range(2) for u in range(2)])

    def own_unit(m, carry):
        hh, other = div(m, 2), rem(m, 2)

        @pl.when(other == 0)
        def _():
            heads_in(hh)

        @pl.when(m == 1)
        def _():
            arrived(stb.at[1 - c], fe_r.at[1])
            build_stats(1 - c)
            arrived(kv.at[pair, 0], kvg_r.at[0, pair])
            spread_all(pair, 0, 3, NEAR, start)

        @pl.when(m == 3)
        def _():
            arrived(kv.at[pair, 1], kvg_r.at[1, pair])
            spread_all(pair, 1, 3, NEAR, start)
            spread_all(s, 1, 0, (1,), start)
            for el in BOTH:
                spread_all(s, el, 0, (2,), start)
                spread_all(pair, el, 3, (2,), start)

        @pl.when(other == 1)
        def _():
            partner_heads_in(hh)

        own_tiles(hh, rem(c + m, 2))
        return carry

    def late_heads(cp):
        lax.fori_loop(2, 4, lambda hh, carry: own_tiles(hh, cp), None)

    send_early()
    lax.fori_loop(0, 4, own_unit, 0)
    for hh in (2, 3):
        heads_in(hh)
    late_heads(c)
    for hh in (2, 3):
        partner_heads_in(hh)

    def acc_y(k, d, kel, m):
        return remote(acc.at[k + 1, kel, m], rxy.at[d, kel, m], ry_s.at[kel, 2 * d + m], ry_r.at[kel, 2 * d + m], across)

    def acc_z(k, d, kel, m):
        to = peer(2 * rem(z + d, 4) + bs)
        return remote(acc.at[k + 1, kel, m], rxz.at[z, kel, m], rz_s.at[kel, 2 * d + m], rz_r.at[kel, 2 * z + m], to)

    def acc_f(k, d, m):
        slot = jnp.where(d == 2, 2, m)
        return remote(acc.at[k + 1, 1, m], rzf.at[slot], zf_s.at[2 * d + m], zf_r.at[slot], peer(2 * rem(z + d, 4) + bs))

    def by_z_first(d, m):
        return ((z == 0) & ((rem(d, 2) == 1) | ((d == 2) & (m == 1)))) | ((z == 1) & (d == 1))

    def step_of(k):
        d, cross = (_pick(z, [_pick(k, [of(name) for name in order]) for order in (*STEPS, STEPS[2])])
                    for of in (lambda name: int(name[1]), lambda name: int(name[0] == "c")))
        g = 2 * rem(z + d, 4) + rem(bs + cross, 2)
        return d, cross, g, div(g - s + 7, 8)

    def pass_at(n):
        for entry in PASS:
            z_lo, z_hi, d, kel = int(entry[0]), int(entry[1]), int(entry[3]), "EL".index(entry[4])
            k = STEPS[min(z_lo, 2)].index(entry[2:4])

            def go_on():
                for m in BOTH:
                    if not (entry.endswith("+") or entry.endswith("v" * m or "-")):
                        arrived(rxy.at[d, kel, m], ry_r.at[kel, 2 * d + m])
                        acc[k + 1, kel, m] += rxy[d, kel, m]
                    acc_z(k, d, kel, m).start()

            pl.when((n == int(entry[5:].rstrip("+v"))) & (z >= z_lo) & (z <= z_hi))(go_on)

    def late_across(k, d):
        def add_in(m, slot):
            arrived(rzf.at[slot], zf_r.at[slot])
            acc[k + 1, 1, m] += rzf[slot]

        @pl.when((d == 0) & (z > 0))
        def _():
            for m in BOTH:
                add_in(m, m)
            pl.when(z == 2)(lambda: add_in(1, 2))

        for m in BOTH:
            zfirst = by_z_first(d, m)
            pl.when(zfirst)(lambda: acc_f(k, d, m).start())
            pl.when(jnp.logical_not(zfirst))(lambda: acc_y(k, d, 1, m).start())

    def heads(p):
        return pl.ds(2 * p, 2)

    def dqx_copy(el, p):
        return remote(dq.at[heads(p), half(1 - c, el), :], dqx.at[el, heads(p)], dqx_s.at[el, p], dqx_r.at[el, p], partner)

    def finish_dq(el, p):
        arrived(dqx.at[el, heads(p)], dqx_r.at[el, p])
        for hh in (2 * p, 2 * p + 1):
            dqs[el, hh] = ((dq[hh, half(c, el), :] + dqx[el, hh]) * SCALE).astype(bf16)
        for t, (dev, _) in enumerate(others):
            remote(dqs.at[el, heads(p), block(el, rem(i + t + 1, 8)), :], dqr.at[h, heads(p), el], odq_s.at[el], odq_r.at[el], dev).start()
        dqr[h, heads(p), el] = dqs[el, heads(p), block(el, i), :]

    def full_unit(n, carry):
        at = jnp.where((z == 3) & (n > 0) & (n < 3), 3 - n, n)
        k, sub = div(at, 2), rem(at, 2)
        d, cross, g, gt = step_of(k)
        el = 1 - sub + sub * gt
        kel = sub * gt

        @pl.when(n == 2)
        def _():
            arrived(qd.at[:, :, seven], qe_r.at[0])
            fw_early().start()
            pl.when(z == 3)(lambda: late_heads(1 - c))

        @pl.when(n == 3 - div(z, 3))
        def _():
            arrived(qd.at[:, :, half(1 - c, 0), :], fe_r.at[0])

        @pl.when((sub == 0) & (d > 0))
        def _():
            arrived(kv.at[g, 0], kvg_r.at[0, g])

        @pl.when((sub == 1) & (d > 0) & (gt == 1))
        def _():
            arrived(kv.at[g, 1], kvg_r.at[1, g])

        bases = [pl.multiple_of(cp * 1024 + el * 512, 512) for cp in (c, 1 - c)]
        tiles(bases, kv.at[g, kel, 0], kv.at[g, kel, 1], acc.at[k + 1, kel, 0], acc.at[k + 1, kel, 1])

        @pl.when((cross == 1) & (sub == gt) & ((gt == 1) | ((d == 0) & (z > 0))))
        def _():
            late_across(k, d)

        @pl.when((cross == 1) & (sub == 1 - gt))
        def _():
            for m in BOTH:
                acc_y(k, d, 0, m).start()

        pass_at(n)

        @pl.when(n == 13 - div(z, 2))
        def _():
            dqx_copy(1, 0).start()
            pl.when(z == 3)(lambda: dqx_copy(1, 1).start())

        return carry

    lax.fori_loop(0, 14, full_unit, 0)

    @pl.when(z >= 2)
    def _():
        finish_dq(1, 0)
        pl.when(z == 3)(lambda: finish_dq(1, 1))

    def diag_unit(m, carry):
        cp = rem(c + 1 + m, 2)
        kd, vd = kv.at[s, 0, 0], kv.at[s, 0, 1]
        tiles([pl.multiple_of(cp * 1024, 512)], kd, vd, acc.at[0, 0, 0], acc.at[0, 0, 1], [(cp, c)])

        @pl.when(m == 0)
        def _():
            for p in BOTH:
                dqx_copy(0, p).start()
            pass_at(14)
            pl.when(z < 2)(lambda: finish_dq(1, 0))

        return carry

    lax.fori_loop(0, 2, diag_unit, 0)
    for p in BOTH:
        finish_dq(0, p)

    @pl.when(z < 3)
    def _():
        late_heads(1 - c)
        dqx_copy(1, 1).start()
        finish_dq(1, 1)


    for el in BOTH:
        for n, got in enumerate((dkr, dvr)):
            def take(ref, rsem):
                arrived(ref, rsem)
                acc[0, el, n] += ref[...]

            for d in AROUND:
                zs = rem(z + d, 4)

                def take_z():
                    take(rxz.at[zs, el, n], rz_r.at[el, 2 * zs + n])

                take_z() if el == 0 else pl.when(z > zs)(take_z)

            def take_y():
                take(rxy.at[0, el, n], ry_r.at[el, n])

            take_y() if el == 0 else pl.when((bs == 1) | (z > 0))(take_y)
            total = jnp.transpose(acc[0, el, n])
            dks[el, n] = (total * SCALE if n == 0 else total).astype(bf16)
            for t, (dev, _) in enumerate(others):
                remote(dks.at[el, n, block(el, rem(i + t + 1, 8)), :], got.at[h, el], odk_s.at[el, n], odk_r.at[el, n], dev).start()
            got[h, el] = dks[el, n, block(el, i), :]

    def by_token(got, el, heads_, wide, out):
        for j in range(heads_):
            wide[pl.ds(j + 64 * el * heads_, 64, stride=heads_), :] = got(j).astype(f32)
        for t in range(64 * el, 64 * el + 64, 16):
            out[pl.ds(t, 16)] = wide[pl.ds(t * heads_, 16 * heads_), :].reshape(16, heads_, out.shape[2]).astype(bf16)

    for el in BOTH:
        arrived(dqr.at[pl.ds(0, 7), :, el], odq_r.at[el])
        by_token(lambda j: dqr[j // 4, j % 4, el], el, 32, wide_q, out_dq)
    for el in BOTH:
        for n, (got, out) in enumerate(((dkr, out_dk), (dvr, out_dv))):
            arrived(got.at[pl.ds(0, 7), el], odk_r.at[el, n])
            by_token(lambda j: got[j, el], el, 8, wide_o, out)

    for n, src in enumerate((k_in, v_in, q_in, do_in, l_in, d_in)):
        sent(src.at[pl.ds(0, 7)], in_s.at[n])
    for el in BOTH:
        to_across(el).wait_send()
        spread_all(s, el, 0, AROUND, lambda cp: cp.wait_send())
        spread_all(pair, el, 3, AROUND, lambda cp: cp.wait_send())
    st_fw.wait_send()
    fw_early().wait_send()
    for hh in range(4):
        fw_late(hh).wait_send()
    for k, name in enumerate(STEPS[0]):
        d, cross = int(name[1]), int(name[0] == "c")
        made = acc_y if cross else acc_z
        later = 2 * rem(z + d, 4) + rem(bs + cross, 2) > s
        if name == "c0":
            later = later | (z > 0)
        for m in BOTH:
            made(k, d, 0, m).wait_send()
            zfirst = by_z_first(d, m) if cross and d > 0 else later & False
            pl.when(later & jnp.logical_not(zfirst))(lambda: made(k, d, 1, m).wait_send())
            if cross and d > 0:
                pl.when(zfirst)(lambda: acc_f(k, d, m).wait_send())
    for el in BOTH:
        for p in BOTH:
            dqx_copy(el, p).wait_send()
        sent(dqs.at[el, :, seven, :], odq_s.at[el])
        for n in BOTH:
            sent(dks.at[el, n, seven, :], odk_s.at[el, n])


def solution(mesh):
    row_spec = P(('dp', 'cy', 'cx'), None, None)
    stat_spec = P(('dp', 'cy', 'cx'), None)

    def local(q, k, v, o, do, lse):
        T, H, D = q.shape
        G = k.shape[1]
        R = H // G
        half = T // 2
        l_in = lse.T.reshape(G, R, T)
        hbm = pl.BlockSpec(memory_space=pl.ANY)
        V, S = pltpu.VMEM, pltpu.SemaphoreType.DMA
        S2, W = 2 * G * T, G * half
        return pl.pallas_call(
            _kernel,
            in_specs=[hbm] * 6,
            out_specs=[pl.BlockSpec(memory_space=pltpu.VMEM)] * 3,
            out_shape=[V((T, H, D), bf16)] + [V((T, G, D), bf16)] * 2,
            scratch_shapes=[
                *[V((T, H, D), bf16)] * 3, *[V((T, G, D), bf16)] * 2, *[V((T * H, D), f32)] * 2,
                *[V((G, 2, R, half, D), bf16)] * 2, *[V((G, 2, half, D), bf16)] * 2, V((G, R, T), f32),
                V((G, R, 2, half, D), bf16), *[V((G, 2, half, D), bf16)] * 2,
                V((2, R, S2, D), bf16), V((2, G, 2, R, T), f32), V((S2, T), f32), V((G, 2, 2, W, D), bf16), V((R, S2, D), f32),
                V((G, 2, 2, D, W), f32), *[V((4, 2, 2, D, W), f32)] * 2, V((3, D, W), f32), V((2, R, W, D), f32),
                V((2, R, W, D), bf16), V((2, 2, W, D), bf16),
                *[S((G,))] * 7, *[S((2, G))] * 10, *[S((2,))] * 8,
            ],
            compiler_params=pltpu.CompilerParams(collective_id=0, has_side_effects=True, vmem_limit_bytes=60 << 20),
            cost_estimate=pl.CostEstimate(flops=46 << 30, bytes_accessed=8 << 20, transcendentals=36 << 20),
            name="attn_bwd",
        )(q, do, o, k, v, l_in)

    return jax.shard_map(local, mesh=mesh, in_specs=(row_spec,) * 5 + (stat_spec,), out_specs=(row_spec,) * 3, check_vma=False)
```

```python
import math
import jax
import jax.numpy as jnp
from jax import lax
from jax.experimental import pallas as pl
from jax.experimental.pallas import tpu as pltpu
from jax.sharding import PartitionSpec as P

f32, bf16 = jnp.float32, jnp.bfloat16
LOG2E = 1.4426950408889634
SCALE = 1.0 / math.sqrt(128.0)
NT = (((1,), (1,)), ((), ()))
TN = (((0,), (0,)), ((), ()))
MESH = pl.DeviceIdType.MESH
BOTH, NEAR, AROUND = (0, 1), (1, 3), (1, 3, 2)
STEPS = (("c1", "s1", "s3", "c3", "c2", "c0", "s2"), ("c1", "c3", "s1", "c2", "s3", "c0", "s2"), ("c1", "c3", "s1", "c2", "s2", "c0", "s3"))
PASS = ("00s3E9", "00s3L5+", "00s1E4", "00s1L3+", "00s2E12", "00s2L14v",
        "12s1E4", "33s1E5", "11s1L5+", "22s1L6", "11s3E9", "11s2E12", "11s2L13", "23s2E10", "23s3E13")

def _pick(k, values):
    r = values[0]
    for n in range(1, len(values)):
        r = jnp.where(k == n, values[n], r)
    return r


def _kernel(q, do, o, k, v, l_in, out_dq, out_dkv,
            qn, don, on, kn, vn, wide_q, wide_o, q_in, do_in, k_in, v_in, d_in, dqr, dkr, dvr,
            qd, stb, st2, kv, dq, acc, rxy, rxz, rzf, dqx, dqs, dks,
            nat_s, in_s, ql_r, fl_s, fl_r, zf_s, zf_r, kvg_s, kvg_r, ry_s, ry_r, rz_s, rz_r, odk_s, odk_r, dqx_s, dqx_r,
            loc_s, kvo_r, st_r, qe_r, fe_s, fe_r, odq_s, odq_r):
    cy, cx = lax.axis_index("cy"), lax.axis_index("cx")
    T = q.shape[0]
    rem, div = lax.rem, lax.div
    x, c = div(cx, 2), rem(cx, 2)
    yl, s = rem(cy, 2), div(cy, 2)
    z, bs = div(s, 2), rem(s, 2)
    a = rem(yl + bs, 2)
    i = yl * 4 + x
    h = a * 4 + x
    pair = 2 * z + 1 - bs

    def member(i2):
        yl2, x2 = div(i2, 4), rem(i2, 4)
        return {"cy": 2 * s + yl2, "cx": 2 * x2 + c}, rem(yl2 + bs, 2) * 4 + x2

    def peer(s2):
        return {"cy": 2 * s2 + rem(a + rem(s2, 2), 2), "cx": cx}

    across = peer(pair)
    partner = {"cy": cy, "cx": cx + 1 - 2 * c}
    others = [member(rem(i + t, 8)) for t in range(1, 8)]
    others_, seven = pl.ds(0, 7), pl.ds(0, 7 * 64)

    def block(el, i2):
        return pl.ds(pl.multiple_of((i2 + el * (7 - 2 * i2)) * 64, 64), 64)

    def half(cp, el):
        return pl.ds(pl.multiple_of(cp * 1024 + el * 512, 512), 512)

    def rows(cp, el, i2):
        return pl.ds(pl.multiple_of(cp * 1024 + el * 512 + (i2 + el * (7 - 2 * i2)) * 64, 64), 64)

    def remote(src, dst, ssem, rsem, dev):
        return pltpu.make_async_remote_copy(src, dst, ssem, rsem, device_id=dev, device_id_type=MESH)

    def arrived(ref, rsem):
        remote(ref, ref, in_s.at[0], rsem, partner).wait_recv()

    def sent(ref, ssem):
        remote(ref, ref, ssem, st_r.at[0], partner).wait_send()

    natives = [pltpu.make_async_copy(src, dst, nat_s.at[n]) for n, (src, dst) in enumerate(((k, kn), (v, vn), (q, qn), (do, don), (o, on)))]
    for cp_ in natives:
        cp_.start()
    pltpu.make_async_copy(l_in.at[h], stb.at[c, i, 0], loc_s.at[0]).start()

    bar = pltpu.get_barrier_semaphore()
    pl.semaphore_signal(bar, inc=1, device_id=partner, device_id_type=MESH)
    pl.semaphore_signal(bar, inc=1, device_id=across, device_id_type=MESH)
    for dev, _ in others:
        pl.semaphore_signal(bar, inc=1, device_id=dev, device_id_type=MESH)
    for d in range(1, 4):
        pl.semaphore_signal(bar, inc=1, device_id=peer(2 * rem(z + d, 4) + bs), device_id_type=MESH)

    def widen(ref, wide):
        heads_ = ref.shape[1]
        for t in range(0, ref.shape[0], 16):
            wide[pl.ds(t * heads_, 16 * heads_), :] = ref[pl.ds(t, 16)].astype(f32).reshape(16 * heads_, ref.shape[2])

    def of_head(wide, j, heads_):
        return wide[pl.ds(j, T, stride=heads_), :]

    for n, (ref, dst) in enumerate(((kn, k_in), (vn, v_in))):
        natives[n].wait()
        widen(ref, wide_o)
        for j in range(8):
            rows_ = of_head(wide_o, j, 8).astype(bf16)
            for el in BOTH:
                dst[j, el] = rows_[64 * el:64 * el + 64]
        for el in BOTH:
            kv[s, el, n, block(el, i), :] = dst[h, el]
    def by_head(n, ref, dst, stats):
        natives[2 + n].wait()
        widen(ref, wide_q)
        if stats:
            natives[4].wait()
            widen(on, wide_o)
        for j in range(32):
            rows_ = of_head(wide_q, j, 32)
            for el in BOTH:
                dst[j // 4, el, j % 4] = rows_[64 * el:64 * el + 64].astype(bf16)
            if stats:
                terms_ = rows_ * of_head(wide_o, j, 32)
                d_in[j // 4, pl.ds(j % 4, 1), :] = jnp.sum(jnp.transpose(terms_), axis=0, keepdims=True)
        for el in BOTH:
            qd[n, :, rows(c, el, i), :] = dst[h, el]

    by_head(0, qn, q_in, False)
    def zero_acc(n, carry):
        acc[n] = jnp.zeros(acc.shape[1:], f32)
        return carry

    lax.fori_loop(0, 8, zero_acc, 0)
    for hh in range(4):
        dq[hh] = jnp.zeros(dq.shape[1:], f32)

    pl.semaphore_wait(bar, 12)
    for el in BOTH:
        for dev, h2 in others:
            for n, src in enumerate((k_in, v_in)):
                remote(src.at[h2, el], kv.at[s, el, n, block(el, i), :], in_s.at[n], kvo_r.at[el], dev).start()
    by_head(1, don, do_in, True)
    stb[c, i, 1] = d_in[h]

    def spread(g, el, d, n):
        return remote(kv.at[g, el], kv.at[g, el], kvg_s.at[el, n], kvg_r.at[el, g], peer(2 * rem(z + 4 - d, 4) + bs))

    def spread_all(g, el, n0, ds, act):
        for d in ds:
            if el == 0:
                act(spread(g, el, d, n0 + d))
            else:
                pl.when(z > rem(z + 4 - d, 4))(lambda: act(spread(g, el, d, n0 + d)))

    def to_across(el):
        return remote(kv.at[s, el], kv.at[s, el], kvg_s.at[el, 0], kvg_r.at[el, s], across)

    def start(cp):
        cp.start()

    def send_stats():
        for dev, h2 in others:
            for n, src in enumerate((l_in, d_in)):
                remote(src.at[h2], stb.at[c, i, n], in_s.at[4 + n], st_r.at[0], dev).start()

    def send_late():
        for hh in range(4):
            for dev, h2 in others:
                for n, src in enumerate((q_in, do_in)):
                    remote(src.at[h2, 1, hh], qd.at[n, hh, rows(c, 1, i), :], in_s.at[2 + n], ql_r.at[hh], dev).start()

    def send_early():
        for dev, h2 in others:
            for n, src in enumerate((q_in, do_in)):
                remote(src.at[h2, 0], qd.at[n, :, rows(c, 0, i), :], in_s.at[2 + n], qe_r.at[0], dev).start()

    for el in BOTH:
        arrived(kv.at[s, el, :, seven], kvo_r.at[el])
        to_across(el).start()
        spread_all(s, el, 0, NEAR if el == 0 else (3,), start)
        if el == 0:
            send_stats()
            send_late()

    def build_stats(cp):
        for i2 in range(8):
            for n, factor in enumerate((LOG2E, 1.0)):
                tile = jnp.transpose(stb[cp, i2, n] * factor)
                for el in BOTH:
                    st2[rows(cp, el, i2), 4 * n:4 * n + 4] = tile[64 * el:64 * el + 64]

    st_fw = remote(stb.at[c], stb.at[c], fe_s.at[1], fe_r.at[1], partner)
    arrived(stb.at[c, others_], st_r.at[0])
    pltpu.make_async_copy(l_in.at[h], stb.at[c, i, 0], loc_s.at[0]).wait()
    st_fw.start()
    build_stats(c)

    def fw_late(hh):
        return remote(qd.at[:, hh, half(c, 1), :], qd.at[:, hh, half(c, 1), :], fl_s.at[hh], fl_r.at[hh], partner)

    def fw_early():
        return remote(qd.at[:, :, half(c, 0), :], qd.at[:, :, half(c, 0), :], fe_s.at[0], fe_r.at[0], partner)

    def scores(hh, r, kref, vref, nk, l2, d, mask=None):
        sc = lax.dot_general(qd[0, hh, r, :], kref[0:nk, :], NT, preferred_element_type=f32)
        dp = lax.dot_general(qd[1, hh, r, :], vref[0:nk, :], NT, preferred_element_type=f32)
        p = jnp.exp2(sc * (SCALE * LOG2E) - l2)
        if mask is not None:
            u, pq, pk = mask
            rr = lax.broadcasted_iota(jnp.int32, (256, nk), 0) + 256 * u
            kk = lax.broadcasted_iota(jnp.int32, (256, nk), 1)
            qpos = (rr >> 6) * 128 + (rr & 63) + pq * 64
            kpos = (kk >> 6) * 128 + (kk & 63) + pk * 64
            p = jnp.where(qpos >= kpos, p, 0.0)
        return p.astype(bf16), (p * (dp - d)).astype(bf16)

    def terms(hh, r, kref, dkref, dvref, nk, pb, ds):
        dkref[:, 0:nk] += lax.dot_general(qd[0, hh, r, :], ds, TN, preferred_element_type=f32)
        dvref[:, 0:nk] += lax.dot_general(qd[1, hh, r, :], pb, TN, preferred_element_type=f32)
        dq[hh, r, :] += jnp.dot(ds, kref[0:nk, :], preferred_element_type=f32)

    def pipelined(todo):
        now = todo[0][0]()
        for n in range(len(todo)):
            nxt = todo[n + 1][0]() if n + 1 < len(todo) else None
            todo[n][1](*now)
            now = nxt

    def tiles(bases, kref, vref, dkref, dvref, masks=None):
        def pair_of(n, hh, u):
            nk = 512 if masks is None or u == 1 else 256
            r = pl.ds(bases[n] + 256 * u, 256)
            mask = None if masks is None else (u, *masks[n])
            return (lambda: scores(hh, r, kref, vref, nk, st2[r, hh:hh + 1], st2[r, 4 + hh:5 + hh], mask),
                    lambda pb, ds: terms(hh, r, kref, dkref, dvref, nk, pb, ds))
        pipelined([pair_of(n, hh, u) for n in range(len(bases)) for u in range(2) for hh in range(4)])

    def heads_in(hh):
        arrived(qd.at[:, hh, seven], ql_r.at[hh])
        fw_late(hh).start()

    def partner_heads_in(hh):
        arrived(qd.at[:, hh, half(1 - c, 1), :], fl_r.at[hh])

    def own_tiles(hh, cp):
        r0 = pl.multiple_of(cp * 1024 + 512, 512)

        def pair_of(el, u):
            nk = 256 if el > u else 512
            r = pl.ds(r0 + 256 * u, 256)
            mask = None if el == 0 else (u, rem(cp + 1, 2), rem(c + 1, 2))
            kref, vref = kv.at[s, el, 0], kv.at[s, el, 1]

            def first():
                st = pltpu.roll(st2[r, :], rem(128 - hh, 128), 1)
                return scores(hh, r, kref, vref, nk, st[:, 0:1], st[:, 4:5], mask)

            return first, lambda pb, ds: terms(hh, r, kref, acc.at[0, el, 0], acc.at[0, el, 1], nk, pb, ds)

        pipelined([pair_of(el, u) for el in range(2) for u in range(2)])

    def own_unit(m, carry):
        hh, other = div(m, 2), rem(m, 2)

        @pl.when(other == 0)
        def _():
            heads_in(hh)

        @pl.when(m == 1)
        def _():
            arrived(stb.at[1 - c], fe_r.at[1])
            build_stats(1 - c)
            arrived(kv.at[pair, 0], kvg_r.at[0, pair])
            spread_all(pair, 0, 3, NEAR, start)

        @pl.when(m == 2)
        def _():
            send_early()

        @pl.when(m == 3)
        def _():
            arrived(kv.at[pair, 1], kvg_r.at[1, pair])
            spread_all(pair, 1, 3, NEAR, start)
            spread_all(s, 1, 0, (1,), start)
            for el in BOTH:
                spread_all(s, el, 0, (2,), start)
                spread_all(pair, el, 3, (2,), start)

        @pl.when(other == 1)
        def _():
            partner_heads_in(hh)

        own_tiles(hh, rem(c + m, 2))
        return carry

    def late_heads(cp):
        lax.fori_loop(2, 4, lambda hh, carry: own_tiles(hh, cp), None)

    lax.fori_loop(0, 4, own_unit, 0)
    for hh in (2, 3):
        heads_in(hh)
    late_heads(c)
    for hh in (2, 3):
        partner_heads_in(hh)

    def acc_y(k, d, kel, m):
        return remote(acc.at[k + 1, kel, m], rxy.at[d, kel, m], ry_s.at[kel, 2 * d + m], ry_r.at[kel, 2 * d + m], across)

    def acc_z(k, d, kel, m):
        to = peer(2 * rem(z + d, 4) + bs)
        return remote(acc.at[k + 1, kel, m], rxz.at[z, kel, m], rz_s.at[kel, 2 * d + m], rz_r.at[kel, 2 * z + m], to)

    def acc_f(k, d, m):
        slot = jnp.where(d == 2, 2, m)
        return remote(acc.at[k + 1, 1, m], rzf.at[slot], zf_s.at[2 * d + m], zf_r.at[slot], peer(2 * rem(z + d, 4) + bs))

    def by_z_first(d, m):
        return ((z == 0) & ((rem(d, 2) == 1) | ((d == 2) & (m == 1)))) | ((z == 1) & (d == 1))

    def step_of(k):
        d, cross = (_pick(z, [_pick(k, [of(name) for name in order]) for order in (*STEPS, STEPS[2])])
                    for of in (lambda name: int(name[1]), lambda name: int(name[0] == "c")))
        g = 2 * rem(z + d, 4) + rem(bs + cross, 2)
        return d, cross, g, div(g - s + 7, 8)

    def pass_at(n):
        for entry in PASS:
            z_lo, z_hi, d, kel = int(entry[0]), int(entry[1]), int(entry[3]), "EL".index(entry[4])
            k = STEPS[min(z_lo, 2)].index(entry[2:4])

            def go_on():
                for m in BOTH:
                    if not (entry.endswith("+") or entry.endswith("v" * m or "-")):
                        arrived(rxy.at[d, kel, m], ry_r.at[kel, 2 * d + m])
                        acc[k + 1, kel, m] += rxy[d, kel, m]
                    acc_z(k, d, kel, m).start()

            pl.when((n == int(entry[5:].rstrip("+v"))) & (z >= z_lo) & (z <= z_hi))(go_on)

    def late_across(k, d):
        def add_in(m, slot):
            arrived(rzf.at[slot], zf_r.at[slot])
            acc[k + 1, 1, m] += rzf[slot]

        @pl.when((d == 0) & (z > 0))
        def _():
            for m in BOTH:
                add_in(m, m)
            pl.when(z == 2)(lambda: add_in(1, 2))

        for m in BOTH:
            zfirst = by_z_first(d, m)
            pl.when(zfirst)(lambda: acc_f(k, d, m).start())
            pl.when(jnp.logical_not(zfirst))(lambda: acc_y(k, d, 1, m).start())

    def heads(p):
        return pl.ds(2 * p, 2)

    def dqx_copy(el, p):
        return remote(dq.at[heads(p), half(1 - c, el), :], dqx.at[el, heads(p)], dqx_s.at[el, p], dqx_r.at[el, p], partner)

    def finish_dq(el, p):
        arrived(dqx.at[el, heads(p)], dqx_r.at[el, p])
        for hh in (2 * p, 2 * p + 1):
            dqs[el, hh] = ((dq[hh, half(c, el), :] + dqx[el, hh]) * SCALE).astype(bf16)
        for t, (dev, _) in enumerate(others):
            remote(dqs.at[el, heads(p), block(el, rem(i + t + 1, 8)), :], dqr.at[h, heads(p), el], odq_s.at[el], odq_r.at[el], dev).start()
        dqr[h, heads(p), el] = dqs[el, heads(p), block(el, i), :]

    def full_unit(n, carry):
        at = jnp.where((z == 3) & (n > 0) & (n < 3), 3 - n, n)
        k, sub = div(at, 2), rem(at, 2)
        d, cross, g, gt = step_of(k)
        el = 1 - sub + sub * gt
        kel = sub * gt

        @pl.when(n == 2)
        def _():
            arrived(qd.at[:, :, seven], qe_r.at[0])
            fw_early().start()
            pl.when(z == 3)(lambda: late_heads(1 - c))

        @pl.when(n == 3 - div(z, 3))
        def _():
            arrived(qd.at[:, :, half(1 - c, 0), :], fe_r.at[0])

        @pl.when((sub == 0) & (d > 0))
        def _():
            arrived(kv.at[g, 0], kvg_r.at[0, g])

        @pl.when((sub == 1) & (d > 0) & (gt == 1))
        def _():
            arrived(kv.at[g, 1], kvg_r.at[1, g])

        bases = [pl.multiple_of(cp * 1024 + el * 512, 512) for cp in (c, 1 - c)]
        tiles(bases, kv.at[g, kel, 0], kv.at[g, kel, 1], acc.at[k + 1, kel, 0], acc.at[k + 1, kel, 1])

        @pl.when((cross == 1) & (sub == gt) & ((gt == 1) | ((d == 0) & (z > 0))))
        def _():
            late_across(k, d)

        @pl.when((cross == 1) & (sub == 1 - gt))
        def _():
            for m in BOTH:
                acc_y(k, d, 0, m).start()

        pass_at(n)

        @pl.when(n == 13 - div(z, 2))
        def _():
            dqx_copy(1, 0).start()
            pl.when(z == 3)(lambda: dqx_copy(1, 1).start())

        return carry

    lax.fori_loop(0, 14, full_unit, 0)

    @pl.when(z >= 2)
    def _():
        finish_dq(1, 0)
        pl.when(z == 3)(lambda: finish_dq(1, 1))

    def diag_unit(m, carry):
        cp = rem(c + 1 + m, 2)
        kd, vd = kv.at[s, 0, 0], kv.at[s, 0, 1]
        tiles([pl.multiple_of(cp * 1024, 512)], kd, vd, acc.at[0, 0, 0], acc.at[0, 0, 1], [(cp, c)])

        @pl.when(m == 0)
        def _():
            for p in BOTH:
                dqx_copy(0, p).start()
            pass_at(14)
            pl.when(z < 2)(lambda: finish_dq(1, 0))

        return carry

    lax.fori_loop(0, 2, diag_unit, 0)
    for p in BOTH:
        finish_dq(0, p)

    @pl.when(z < 3)
    def _():
        late_heads(1 - c)
        dqx_copy(1, 1).start()
        finish_dq(1, 1)


    for el in BOTH:
        for n, got in enumerate((dkr, dvr)):
            def take(ref, rsem):
                arrived(ref, rsem)
                acc[0, el, n] += ref[...]

            for d in AROUND:
                zs = rem(z + d, 4)

                def take_z():
                    take(rxz.at[zs, el, n], rz_r.at[el, 2 * zs + n])

                take_z() if el == 0 else pl.when(z > zs)(take_z)

            def take_y():
                take(rxy.at[0, el, n], ry_r.at[el, n])

            take_y() if el == 0 else pl.when((bs == 1) | (z > 0))(take_y)
            total = jnp.transpose(acc[0, el, n])
            dks[el, n] = (total * SCALE if n == 0 else total).astype(bf16)
            for t, (dev, _) in enumerate(others):
                remote(dks.at[el, n, block(el, rem(i + t + 1, 8)), :], got.at[h, el], odk_s.at[el, n], odk_r.at[el, n], dev).start()
            got[h, el] = dks[el, n, block(el, i), :]

    def by_token(got, el, heads_, wide, out, first=0):
        for j in range(heads_):
            wide[pl.ds(j + 64 * el * heads_, 64, stride=heads_), :] = got(j).astype(f32)
        for t in range(64 * el, 64 * el + 64, 16):
            out[pl.ds(t, 16), first:first + heads_] = wide[pl.ds(t * heads_, 16 * heads_), :].reshape(16, heads_, out.shape[2]).astype(bf16)

    for el in BOTH:
        arrived(dqr.at[others_, :, el], odq_r.at[el])
        by_token(lambda j: dqr[j // 4, j % 4, el], el, 32, wide_q, out_dq)
    for el in BOTH:
        for n, got in enumerate((dkr, dvr)):
            arrived(got.at[others_, el], odk_r.at[el, n])
            by_token(lambda j: got[j, el], el, 8, wide_o, out_dkv, 8 * n)

    for n, src in enumerate((k_in, v_in, q_in, do_in, l_in, d_in)):
        sent(src.at[others_], in_s.at[n])
    for el in BOTH:
        to_across(el).wait_send()
        spread_all(s, el, 0, AROUND, lambda cp: cp.wait_send())
        spread_all(pair, el, 3, AROUND, lambda cp: cp.wait_send())
    st_fw.wait_send()
    fw_early().wait_send()
    for hh in range(4):
        fw_late(hh).wait_send()
    for k, name in enumerate(STEPS[0]):
        d, cross = int(name[1]), int(name[0] == "c")
        made = acc_y if cross else acc_z
        later = 2 * rem(z + d, 4) + rem(bs + cross, 2) > s
        if name == "c0":
            later = later | (z > 0)
        for m in BOTH:
            made(k, d, 0, m).wait_send()
            zfirst = by_z_first(d, m) if cross and d > 0 else later & False
            pl.when(later & jnp.logical_not(zfirst))(lambda: made(k, d, 1, m).wait_send())
            if cross and d > 0:
                pl.when(zfirst)(lambda: acc_f(k, d, m).wait_send())
    for el in BOTH:
        for p in BOTH:
            dqx_copy(el, p).wait_send()
        sent(dqs.at[el, :, seven, :], odq_s.at[el])
        for n in BOTH:
            sent(dks.at[el, n, seven, :], odk_s.at[el, n])


def solution(mesh):
    row_spec = P(('dp', 'cy', 'cx'), None, None)
    stat_spec = P(('dp', 'cy', 'cx'), None)

    def local(q, k, v, o, do, lse):
        T, H, D = q.shape
        G = k.shape[1]
        R = H // G
        half = T // 2
        l_in = lse.T.reshape(G, R, T)
        hbm = pl.BlockSpec(memory_space=pl.ANY)
        V, S = pltpu.VMEM, pltpu.SemaphoreType.DMA
        S2, W = 2 * G * T, G * half
        grad_q, grad_kv = pl.pallas_call(
            _kernel,
            in_specs=[hbm] * 6,
            out_specs=[pl.BlockSpec(memory_space=pltpu.VMEM)] * 2,
            out_shape=[V((T, H, D), bf16), V((T, 2 * G, D), bf16)],
            scratch_shapes=[
                *[V((T, H, D), bf16)] * 3, *[V((T, G, D), bf16)] * 2, *[V((T * H, D), f32)] * 2,
                *[V((G, 2, R, half, D), bf16)] * 2, *[V((G, 2, half, D), bf16)] * 2, V((G, R, T), f32),
                V((G, R, 2, half, D), bf16), *[V((G, 2, half, D), bf16)] * 2,
                V((2, R, S2, D), bf16), V((2, G, 2, R, T), f32), V((S2, T), f32), V((G, 2, 2, W, D), bf16), V((R, S2, D), f32),
                V((G, 2, 2, D, W), f32), *[V((4, 2, 2, D, W), f32)] * 2, V((3, D, W), f32), V((2, R, W, D), f32),
                V((2, R, W, D), bf16), V((2, 2, W, D), bf16),
                *[S((G,))] * 7, *[S((2, G))] * 10, *[S((2,))] * 8,
            ],
            compiler_params=pltpu.CompilerParams(collective_id=0, has_side_effects=True, vmem_limit_bytes=60 << 20),
            cost_estimate=pl.CostEstimate(flops=46 << 30, bytes_accessed=8 << 20, transcendentals=36 << 20),
            name="attn_bwd",
        )(q, do, o, k, v, l_in)
        return grad_q, grad_kv[:, :G], grad_kv[:, G:]

    return jax.shard_map(local, mesh=mesh, in_specs=(row_spec,) * 5 + (stat_spec,), out_specs=(row_spec,) * 3, check_vma=False)
```

```python
import math
import jax
import jax.numpy as jnp
from jax import lax
from jax.experimental import pallas as pl
from jax.experimental.pallas import tpu as pltpu
from jax.sharding import PartitionSpec as P

f32, bf16 = jnp.float32, jnp.bfloat16
LOG2E = 1.4426950408889634
SCALE = 1.0 / math.sqrt(128.0)
NT = (((1,), (1,)), ((), ()))
TN = (((0,), (0,)), ((), ()))
MESH = pl.DeviceIdType.MESH
BOTH, NEAR, AROUND = (0, 1), (1, 3), (1, 3, 2)
STEPS = (("c1", "s1", "s3", "c3", "c2", "c0", "s2"), ("c1", "c3", "s1", "c2", "s3", "c0", "s2"), ("c1", "c3", "s1", "c2", "s2", "c0", "s3"))
PASS = ("00s3E9", "00s3L5+", "00s1E4", "00s1L3+", "00s2E12", "00s2L13v",
        "12s1E4", "33s1E5", "11s1L5+", "22s1L6", "11s3E9", "11s2E12", "11s2L13", "23s2E10", "23s3E13")

def _pick(k, values):
    r = values[0]
    for n in range(1, len(values)):
        r = jnp.where(k == n, values[n], r)
    return r


def _kernel(q, do, o, k, v, l_in, out_dq, out_dkv,
            qn, don, on, kn, vn, wide_q, wide_o, q_in, do_in, k_in, v_in, d_in, dqr, dkr, dvr,
            qd, stb, st2, kv, dq, acc, rxy, rxz, rzf, dqx, dqs, dks,
            nat_s, in_s, ql_r, fl_s, fl_r, zf_s, zf_r, kvg_s, kvg_r, ry_s, ry_r, rz_s, rz_r, odk_s, odk_r, dqx_s, dqx_r,
            loc_s, kvo_r, st_r, qe_r, fe_s, fe_r, odq_s, odq_r):
    cy, cx = lax.axis_index("cy"), lax.axis_index("cx")
    T = q.shape[0]
    rem, div = lax.rem, lax.div
    x, c = div(cx, 2), rem(cx, 2)
    yl, s = rem(cy, 2), div(cy, 2)
    z, bs = div(s, 2), rem(s, 2)
    a = rem(yl + bs, 2)
    i = yl * 4 + x
    h = a * 4 + x
    pair = 2 * z + 1 - bs

    def member(i2):
        yl2, x2 = div(i2, 4), rem(i2, 4)
        return {"cy": 2 * s + yl2, "cx": 2 * x2 + c}, rem(yl2 + bs, 2) * 4 + x2

    def peer(s2):
        return {"cy": 2 * s2 + rem(a + rem(s2, 2), 2), "cx": cx}

    across = peer(pair)
    partner = {"cy": cy, "cx": cx + 1 - 2 * c}
    others = [member(rem(i + t, 8)) for t in range(1, 8)]
    others_, seven = pl.ds(0, 7), pl.ds(0, 7 * 64)

    def block(el, i2):
        return pl.ds(pl.multiple_of((i2 + el * (7 - 2 * i2)) * 64, 64), 64)

    def half(cp, el):
        return pl.ds(pl.multiple_of(cp * 1024 + el * 512, 512), 512)

    def rows(cp, el, i2):
        return pl.ds(pl.multiple_of(cp * 1024 + el * 512 + (i2 + el * (7 - 2 * i2)) * 64, 64), 64)

    def remote(src, dst, ssem, rsem, dev):
        return pltpu.make_async_remote_copy(src, dst, ssem, rsem, device_id=dev, device_id_type=MESH)

    def arrived(ref, rsem):
        remote(ref, ref, in_s.at[0], rsem, partner).wait_recv()

    def sent(ref, ssem):
        remote(ref, ref, ssem, st_r.at[0], partner).wait_send()

    natives = [pltpu.make_async_copy(src, dst, nat_s.at[n]) for n, (src, dst) in enumerate(((k, kn), (v, vn), (q, qn), (do, don), (o, on)))]
    for cp_ in natives:
        cp_.start()
    pltpu.make_async_copy(l_in.at[h], stb.at[c, i, 0], loc_s.at[0]).start()

    bar = pltpu.get_barrier_semaphore()
    pl.semaphore_signal(bar, inc=1, device_id=partner, device_id_type=MESH)
    pl.semaphore_signal(bar, inc=1, device_id=across, device_id_type=MESH)
    for dev, _ in others:
        pl.semaphore_signal(bar, inc=1, device_id=dev, device_id_type=MESH)
    for d in range(1, 4):
        pl.semaphore_signal(bar, inc=1, device_id=peer(2 * rem(z + d, 4) + bs), device_id_type=MESH)

    def widen(ref, wide):
        heads_ = ref.shape[1]
        for t in range(0, ref.shape[0], 16):
            wide[pl.ds(t * heads_, 16 * heads_), :] = ref[pl.ds(t, 16)].astype(f32).reshape(16 * heads_, ref.shape[2])

    def of_head(wide, j, heads_):
        return wide[pl.ds(j, T, stride=heads_), :]

    for n, (ref, dst) in enumerate(((kn, k_in), (vn, v_in))):
        natives[n].wait()
        widen(ref, wide_o)
        for j in range(8):
            rows_ = of_head(wide_o, j, 8).astype(bf16)
            for el in BOTH:
                dst[j, el] = rows_[64 * el:64 * el + 64]
        for el in BOTH:
            kv[s, el, n, block(el, i), :] = dst[h, el]
    def by_head(n, ref, dst, stats):
        natives[2 + n].wait()
        widen(ref, wide_q)
        if stats:
            natives[4].wait()
            widen(on, wide_o)
        for j in range(32):
            rows_ = of_head(wide_q, j, 32)
            for el in BOTH:
                dst[j // 4, el, j % 4] = rows_[64 * el:64 * el + 64].astype(bf16)
            if stats:
                terms_ = rows_ * of_head(wide_o, j, 32)
                d_in[j // 4, pl.ds(j % 4, 1), :] = jnp.sum(jnp.transpose(terms_), axis=0, keepdims=True)
        for el in BOTH:
            qd[n, :, rows(c, el, i), :] = dst[h, el]

    by_head(0, qn, q_in, False)
    def zero_acc(n, carry):
        acc[n] = jnp.zeros(acc.shape[1:], f32)
        return carry

    lax.fori_loop(0, 8, zero_acc, 0)
    for hh in range(4):
        dq[hh] = jnp.zeros(dq.shape[1:], f32)

    pl.semaphore_wait(bar, 12)
    for el in BOTH:
        for dev, h2 in others:
            for n, src in enumerate((k_in, v_in)):
                remote(src.at[h2, el], kv.at[s, el, n, block(el, i), :], in_s.at[n], kvo_r.at[el], dev).start()
    by_head(1, don, do_in, True)
    stb[c, i, 1] = d_in[h]

    def spread(g, el, d, n):
        return remote(kv.at[g, el], kv.at[g, el], kvg_s.at[el, n], kvg_r.at[el, g], peer(2 * rem(z + 4 - d, 4) + bs))

    def spread_all(g, el, n0, ds, act):
        for d in ds:
            if el == 0:
                act(spread(g, el, d, n0 + d))
            else:
                pl.when(z > rem(z + 4 - d, 4))(lambda: act(spread(g, el, d, n0 + d)))

    def to_across(el):
        return remote(kv.at[s, el], kv.at[s, el], kvg_s.at[el, 0], kvg_r.at[el, s], across)

    def start(cp):
        cp.start()

    def send_stats():
        for dev, h2 in others:
            for n, src in enumerate((l_in, d_in)):
                remote(src.at[h2], stb.at[c, i, n], in_s.at[4 + n], st_r.at[0], dev).start()

    def send_late():
        for hh in range(4):
            for dev, h2 in others:
                for n, src in enumerate((q_in, do_in)):
                    remote(src.at[h2, 1, hh], qd.at[n, hh, rows(c, 1, i), :], in_s.at[2 + n], ql_r.at[hh], dev).start()

    def send_early():
        for dev, h2 in others:
            for n, src in enumerate((q_in, do_in)):
                remote(src.at[h2, 0], qd.at[n, :, rows(c, 0, i), :], in_s.at[2 + n], qe_r.at[0], dev).start()

    for el in BOTH:
        arrived(kv.at[s, el, :, seven], kvo_r.at[el])
        to_across(el).start()
        spread_all(s, el, 0, NEAR if el == 0 else (3,), start)
        if el == 0:
            send_stats()
            send_late()

    def build_stats(cp):
        for i2 in range(8):
            for n, factor in enumerate((LOG2E, 1.0)):
                tile = jnp.transpose(stb[cp, i2, n] * factor)
                for el in BOTH:
                    st2[rows(cp, el, i2), 4 * n:4 * n + 4] = tile[64 * el:64 * el + 64]

    st_fw = remote(stb.at[c], stb.at[c], fe_s.at[1], fe_r.at[1], partner)
    arrived(stb.at[c, others_], st_r.at[0])
    pltpu.make_async_copy(l_in.at[h], stb.at[c, i, 0], loc_s.at[0]).wait()
    st_fw.start()
    build_stats(c)

    def fw_late(hh):
        return remote(qd.at[:, hh, half(c, 1), :], qd.at[:, hh, half(c, 1), :], fl_s.at[hh], fl_r.at[hh], partner)

    def fw_early():
        return remote(qd.at[:, :, half(c, 0), :], qd.at[:, :, half(c, 0), :], fe_s.at[0], fe_r.at[0], partner)

    def scores(hh, r, kref, vref, nk, l2, d, mask=None):
        sc = lax.dot_general(qd[0, hh, r, :], kref[0:nk, :], NT, preferred_element_type=f32)
        dp = lax.dot_general(qd[1, hh, r, :], vref[0:nk, :], NT, preferred_element_type=f32)
        p = jnp.exp2(sc * (SCALE * LOG2E) - l2)
        if mask is not None:
            u, pq, pk = mask
            rr = lax.broadcasted_iota(jnp.int32, (256, nk), 0) + 256 * u
            kk = lax.broadcasted_iota(jnp.int32, (256, nk), 1)
            qpos = (rr >> 6) * 128 + (rr & 63) + pq * 64
            kpos = (kk >> 6) * 128 + (kk & 63) + pk * 64
            p = jnp.where(qpos >= kpos, p, 0.0)
        return p.astype(bf16), (p * (dp - d)).astype(bf16)

    def terms(hh, r, kref, dkref, dvref, nk, pb, ds):
        dkref[:, 0:nk] += lax.dot_general(qd[0, hh, r, :], ds, TN, preferred_element_type=f32)
        dvref[:, 0:nk] += lax.dot_general(qd[1, hh, r, :], pb, TN, preferred_element_type=f32)
        dq[hh, r, :] += jnp.dot(ds, kref[0:nk, :], preferred_element_type=f32)

    def pipelined(todo):
        now = todo[0][0]()
        for n in range(len(todo)):
            nxt = todo[n + 1][0]() if n + 1 < len(todo) else None
            todo[n][1](*now)
            now = nxt

    def tiles(bases, kref, vref, dkref, dvref, masks=None):
        def pair_of(n, hh, u):
            nk = 512 if masks is None or u == 1 else 256
            r = pl.ds(bases[n] + 256 * u, 256)
            mask = None if masks is None else (u, *masks[n])
            return (lambda: scores(hh, r, kref, vref, nk, st2[r, hh:hh + 1], st2[r, 4 + hh:5 + hh], mask),
                    lambda pb, ds: terms(hh, r, kref, dkref, dvref, nk, pb, ds))
        pipelined([pair_of(n, hh, u) for n in range(len(bases)) for u in range(2) for hh in range(4)])

    def heads_in(hh):
        arrived(qd.at[:, hh, seven], ql_r.at[hh])
        fw_late(hh).start()

    def partner_heads_in(hh):
        arrived(qd.at[:, hh, half(1 - c, 1), :], fl_r.at[hh])

    def own_tiles(hh, cp):
        r0 = pl.multiple_of(cp * 1024 + 512, 512)

        def pair_of(el, u):
            nk = 256 if el > u else 512
            r = pl.ds(r0 + 256 * u, 256)
            mask = None if el == 0 else (u, rem(cp + 1, 2), rem(c + 1, 2))
            kref, vref = kv.at[s, el, 0], kv.at[s, el, 1]

            def first():
                st = pltpu.roll(st2[r, :], rem(128 - hh, 128), 1)
                return scores(hh, r, kref, vref, nk, st[:, 0:1], st[:, 4:5], mask)

            return first, lambda pb, ds: terms(hh, r, kref, acc.at[0, el, 0], acc.at[0, el, 1], nk, pb, ds)

        pipelined([pair_of(el, u) for el in range(2) for u in range(2)])

    def own_unit(m, carry):
        hh, other = div(m, 2), rem(m, 2)

        @pl.when(other == 0)
        def _():
            heads_in(hh)

        @pl.when(m == 1)
        def _():
            arrived(stb.at[1 - c], fe_r.at[1])
            build_stats(1 - c)
            arrived(kv.at[pair, 0], kvg_r.at[0, pair])
            spread_all(pair, 0, 3, NEAR, start)

        @pl.when(m == 2)
        def _():
            send_early()

        @pl.when(m == 3)
        def _():
            arrived(kv.at[pair, 1], kvg_r.at[1, pair])
            spread_all(pair, 1, 3, NEAR, start)
            spread_all(s, 1, 0, (1,), start)
            for el in BOTH:
                spread_all(s, el, 0, (2,), start)
                spread_all(pair, el, 3, (2,), start)

        @pl.when(other == 1)
        def _():
            partner_heads_in(hh)

        own_tiles(hh, rem(c + m, 2))
        return carry

    def late_heads(cp):
        lax.fori_loop(2, 4, lambda hh, carry: own_tiles(hh, cp), None)

    lax.fori_loop(0, 4, own_unit, 0)
    for hh in (2, 3):
        heads_in(hh)
    late_heads(c)
    for hh in (2, 3):
        partner_heads_in(hh)

    def acc_y(k, d, kel, m):
        return remote(acc.at[k + 1, kel, m], rxy.at[d, kel, m], ry_s.at[kel, 2 * d + m], ry_r.at[kel, 2 * d + m], across)

    def acc_z(k, d, kel, m):
        to = peer(2 * rem(z + d, 4) + bs)
        return remote(acc.at[k + 1, kel, m], rxz.at[z, kel, m], rz_s.at[kel, 2 * d + m], rz_r.at[kel, 2 * z + m], to)

    def acc_f(k, d, m):
        slot = jnp.where(d == 2, 2, m)
        return remote(acc.at[k + 1, 1, m], rzf.at[slot], zf_s.at[2 * d + m], zf_r.at[slot], peer(2 * rem(z + d, 4) + bs))

    def by_z_first(d, m):
        return ((z == 0) & ((rem(d, 2) == 1) | ((d == 2) & (m == 1)))) | ((z == 1) & (d == 1))

    def step_of(k):
        d, cross = (_pick(z, [_pick(k, [of(name) for name in order]) for order in (*STEPS, STEPS[2])])
                    for of in (lambda name: int(name[1]), lambda name: int(name[0] == "c")))
        g = 2 * rem(z + d, 4) + rem(bs + cross, 2)
        return d, cross, g, div(g - s + 7, 8)

    def pass_at(n):
        for entry in PASS:
            z_lo, z_hi, d, kel = int(entry[0]), int(entry[1]), int(entry[3]), "EL".index(entry[4])
            k = STEPS[min(z_lo, 2)].index(entry[2:4])

            def go_on():
                for m in BOTH:
                    if not (entry.endswith("+") or entry.endswith("v" * m or "-")):
                        arrived(rxy.at[d, kel, m], ry_r.at[kel, 2 * d + m])
                        acc[k + 1, kel, m] += rxy[d, kel, m]
                    acc_z(k, d, kel, m).start()

            pl.when((n == int(entry[5:].rstrip("+v"))) & (z >= z_lo) & (z <= z_hi))(go_on)

    def late_across(k, d):
        def add_in(m, slot):
            arrived(rzf.at[slot], zf_r.at[slot])
            acc[k + 1, 1, m] += rzf[slot]

        @pl.when((d == 0) & (z > 0))
        def _():
            for m in BOTH:
                add_in(m, m)
            pl.when(z == 2)(lambda: add_in(1, 2))

        for m in BOTH:
            zfirst = by_z_first(d, m)
            pl.when(zfirst)(lambda: acc_f(k, d, m).start())
            pl.when(jnp.logical_not(zfirst))(lambda: acc_y(k, d, 1, m).start())

    def heads(p):
        return pl.ds(2 * p, 2)

    def dqx_copy(el, p):
        return remote(dq.at[heads(p), half(1 - c, el), :], dqx.at[el, heads(p)], dqx_s.at[el, p], dqx_r.at[el, p], partner)

    def finish_dq(el, p):
        arrived(dqx.at[el, heads(p)], dqx_r.at[el, p])
        for hh in (2 * p, 2 * p + 1):
            dqs[el, hh] = ((dq[hh, half(c, el), :] + dqx[el, hh]) * SCALE).astype(bf16)
        for t, (dev, _) in enumerate(others):
            remote(dqs.at[el, heads(p), block(el, rem(i + t + 1, 8)), :], dqr.at[h, heads(p), el], odq_s.at[el], odq_r.at[el], dev).start()
        dqr[h, heads(p), el] = dqs[el, heads(p), block(el, i), :]

    def full_unit(n, carry):
        at = jnp.where((z == 3) & (n > 0) & (n < 3), 3 - n, n)
        k, sub = div(at, 2), rem(at, 2)
        d, cross, g, gt = step_of(k)
        el = 1 - sub + sub * gt
        kel = sub * gt

        @pl.when(n == 2)
        def _():
            arrived(qd.at[:, :, seven], qe_r.at[0])
            fw_early().start()
            pl.when(z == 3)(lambda: late_heads(1 - c))

        @pl.when(n == 3 - div(z, 3))
        def _():
            arrived(qd.at[:, :, half(1 - c, 0), :], fe_r.at[0])

        @pl.when((sub == 0) & (d > 0))
        def _():
            arrived(kv.at[g, 0], kvg_r.at[0, g])

        @pl.when((sub == 1) & (d > 0) & (gt == 1))
        def _():
            arrived(kv.at[g, 1], kvg_r.at[1, g])

        bases = [pl.multiple_of(cp * 1024 + el * 512, 512) for cp in (c, 1 - c)]
        tiles(bases, kv.at[g, kel, 0], kv.at[g, kel, 1], acc.at[k + 1, kel, 0], acc.at[k + 1, kel, 1])

        @pl.when((cross == 1) & (sub == gt) & ((gt == 1) | ((d == 0) & (z > 0))))
        def _():
            late_across(k, d)

        @pl.when((cross == 1) & (sub == 1 - gt))
        def _():
            for m in BOTH:
                acc_y(k, d, 0, m).start()

        pass_at(n)

        @pl.when(n == 13 - div(z, 2))
        def _():
            dqx_copy(1, 0).start()
            pl.when(z == 3)(lambda: dqx_copy(1, 1).start())

        return carry

    lax.fori_loop(0, 14, full_unit, 0)

    @pl.when(z >= 2)
    def _():
        finish_dq(1, 0)
        pl.when(z == 3)(lambda: finish_dq(1, 1))

    def diag_unit(m, carry):
        cp = rem(c + 1 + m, 2)
        kd, vd = kv.at[s, 0, 0], kv.at[s, 0, 1]
        tiles([pl.multiple_of(cp * 1024, 512)], kd, vd, acc.at[0, 0, 0], acc.at[0, 0, 1], [(cp, c)])

        @pl.when(m == 0)
        def _():
            for p in BOTH:
                dqx_copy(0, p).start()
            pass_at(14)
            pl.when(z < 2)(lambda: finish_dq(1, 0))

        return carry

    lax.fori_loop(0, 2, diag_unit, 0)
    for p in BOTH:
        finish_dq(0, p)

    @pl.when(z < 3)
    def _():
        late_heads(1 - c)
        dqx_copy(1, 1).start()
        finish_dq(1, 1)


    for el in BOTH:
        for n, got in enumerate((dkr, dvr)):
            def take(ref, rsem):
                arrived(ref, rsem)
                acc[0, el, n] += ref[...]

            for d in AROUND:
                zs = rem(z + d, 4)

                def take_z():
                    take(rxz.at[zs, el, n], rz_r.at[el, 2 * zs + n])

                take_z() if el == 0 else pl.when(z > zs)(take_z)

            def take_y():
                take(rxy.at[0, el, n], ry_r.at[el, n])

            take_y() if el == 0 else pl.when((bs == 1) | (z > 0))(take_y)
            total = jnp.transpose(acc[0, el, n])
            dks[el, n] = (total * SCALE if n == 0 else total).astype(bf16)
            for t, (dev, _) in enumerate(others):
                remote(dks.at[el, n, block(el, rem(i + t + 1, 8)), :], got.at[h, el], odk_s.at[el, n], odk_r.at[el, n], dev).start()
            got[h, el] = dks[el, n, block(el, i), :]

    def by_token(got, el, heads_, wide, out, first=0):
        for j in range(heads_):
            wide[pl.ds(j + 64 * el * heads_, 64, stride=heads_), :] = got(j).astype(f32)
        for t in range(64 * el, 64 * el + 64, 16):
            out[pl.ds(t, 16), first:first + heads_] = wide[pl.ds(t * heads_, 16 * heads_), :].reshape(16, heads_, out.shape[2]).astype(bf16)

    for el in BOTH:
        arrived(dqr.at[others_, :, el], odq_r.at[el])
        by_token(lambda j: dqr[j // 4, j % 4, el], el, 32, wide_q, out_dq)
    for el in BOTH:
        for n, got in enumerate((dkr, dvr)):
            arrived(got.at[others_, el], odk_r.at[el, n])
            by_token(lambda j: got[j, el], el, 8, wide_o, out_dkv, 8 * n)

    for n, src in enumerate((k_in, v_in, q_in, do_in, l_in, d_in)):
        sent(src.at[others_], in_s.at[n])
    for el in BOTH:
        to_across(el).wait_send()
        spread_all(s, el, 0, AROUND, lambda cp: cp.wait_send())
        spread_all(pair, el, 3, AROUND, lambda cp: cp.wait_send())
    st_fw.wait_send()
    fw_early().wait_send()
    for hh in range(4):
        fw_late(hh).wait_send()
    for k, name in enumerate(STEPS[0]):
        d, cross = int(name[1]), int(name[0] == "c")
        made = acc_y if cross else acc_z
        later = 2 * rem(z + d, 4) + rem(bs + cross, 2) > s
        if name == "c0":
            later = later | (z > 0)
        for m in BOTH:
            made(k, d, 0, m).wait_send()
            zfirst = by_z_first(d, m) if cross and d > 0 else later & False
            pl.when(later & jnp.logical_not(zfirst))(lambda: made(k, d, 1, m).wait_send())
            if cross and d > 0:
                pl.when(zfirst)(lambda: acc_f(k, d, m).wait_send())
    for el in BOTH:
        for p in BOTH:
            dqx_copy(el, p).wait_send()
        sent(dqs.at[el, :, seven, :], odq_s.at[el])
        for n in BOTH:
            sent(dks.at[el, n, seven, :], odk_s.at[el, n])


def solution(mesh):
    row_spec = P(('dp', 'cy', 'cx'), None, None)
    stat_spec = P(('dp', 'cy', 'cx'), None)

    def local(q, k, v, o, do, lse):
        T, H, D = q.shape
        G = k.shape[1]
        R = H // G
        half = T // 2
        l_in = lse.T.reshape(G, R, T)
        hbm = pl.BlockSpec(memory_space=pl.ANY)
        V, S = pltpu.VMEM, pltpu.SemaphoreType.DMA
        S2, W = 2 * G * T, G * half
        grad_q, grad_kv = pl.pallas_call(
            _kernel,
            in_specs=[hbm] * 6,
            out_specs=[pl.BlockSpec(memory_space=pltpu.VMEM)] * 2,
            out_shape=[V((T, H, D), bf16), V((T, 2 * G, D), bf16)],
            scratch_shapes=[
                *[V((T, H, D), bf16)] * 3, *[V((T, G, D), bf16)] * 2, *[V((T * H, D), f32)] * 2,
                *[V((G, 2, R, half, D), bf16)] * 2, *[V((G, 2, half, D), bf16)] * 2, V((G, R, T), f32),
                V((G, R, 2, half, D), bf16), *[V((G, 2, half, D), bf16)] * 2,
                V((2, R, S2, D), bf16), V((2, G, 2, R, T), f32), V((S2, T), f32), V((G, 2, 2, W, D), bf16), V((R, S2, D), f32),
                V((G, 2, 2, D, W), f32), *[V((4, 2, 2, D, W), f32)] * 2, V((3, D, W), f32), V((2, R, W, D), f32),
                V((2, R, W, D), bf16), V((2, 2, W, D), bf16),
                *[S((G,))] * 7, *[S((2, G))] * 10, *[S((2,))] * 8,
            ],
            compiler_params=pltpu.CompilerParams(collective_id=0, has_side_effects=True, vmem_limit_bytes=60 << 20),
            cost_estimate=pl.CostEstimate(flops=46 << 30, bytes_accessed=8 << 20, transcendentals=36 << 20),
            name="attn_bwd",
        )(q, do, o, k, v, l_in)
        return grad_q, grad_kv[:, :G], grad_kv[:, G:]

    return jax.shard_map(local, mesh=mesh, in_specs=(row_spec,) * 5 + (stat_spec,), out_specs=(row_spec,) * 3, check_vma=False)
```
